16 devices in a mesh: dp: 2 (over y, z), ep: 8 (over x, core).
Axes of the slice: x: 4, y: 2, z: 1, core: 2. Of those that a mesh axis runs over, the one named last changes fastest.
The devices are a block of a 4x4x8 slice.
Arguments:
- x_rows: bfloat16 [8192, 2048], P(('dp', 'ep')), parts along dimension 0
- logits: float32 [8192, 256], P(('dp', 'ep')), parts along dimension 0
- w_in: bfloat16 [256, 2048, 512], P('ep')
- w_out: bfloat16 [256, 512, 2048], P('ep')
- shared_in: bfloat16 [2048, 512], replicated
- shared_out: bfloat16 [512, 2048], replicated
Outputs:
- output: bfloat16 [8192, 2048], P(('dp', 'ep')), parts along dimension 0
There are 2 independent parts. The reference program is written for one: setup_inputs(seed, part) draws one part's arguments, and reference() takes and returns one part's arrays. A program takes and returns all parts, laid end to end along the dimension named above; an argument that names none is the same for every part.
All inputs are finite; a program needn't handle non-finite values.
Results may differ from the reference program's by a relative error of at most 0.00543669.
Values are sent between devices in bfloat16 or wider.
A program may use at most 768 MiB of HBM per device.

```python
import jax
import jax.numpy as jnp
import numpy as np
from jax import lax

TOK_DEV = 512
GROUP_SIZE = 8
D_MODEL = 2048
FF_EXPERT = 512
FF_SHARED = 512
EXPERTS = 256
CAP_FACTOR = 2

TOKENS = TOK_DEV * GROUP_SIZE
LOCAL_EXPERTS = EXPERTS // GROUP_SIZE
CAPACITY = TOKENS * CAP_FACTOR // EXPERTS
PAIR_CAP = 2 * TOK_DEV * CAP_FACTOR // GROUP_SIZE
LOGIT_MULT = max(1, 131072 // TOKENS)


def draw_logits(route_key):
    slot_start = np.arange(LOCAL_EXPERTS)[:, None] * CAPACITY
    src_start = np.arange(GROUP_SIZE)[None, :] * PAIR_CAP
    common_len = np.minimum(slot_start + CAPACITY, src_start + PAIR_CAP) - np.maximum(slot_start, src_start)
    count_table = jnp.asarray(np.maximum(common_len, 0), dtype=jnp.int32)
    k_owner, k_local, k_column = jax.random.split(route_key, 3)
    owner_perm = jax.random.permutation(k_owner, jnp.broadcast_to(jnp.arange(GROUP_SIZE), (GROUP_SIZE, GROUP_SIZE)), axis=1, independent=True)
    counts = jnp.transpose(count_table[:, owner_perm], (1, 0, 2)).reshape(EXPERTS, GROUP_SIZE, 1)
    local_rank = jax.random.permutation(k_local, jnp.broadcast_to(jnp.arange(TOK_DEV), (EXPERTS, GROUP_SIZE, TOK_DEV)), axis=2, independent=True)
    chosen = (local_rank < counts).reshape(EXPERTS, TOKENS).astype(jnp.int32)
    column_perm = jax.random.permutation(k_column, jnp.broadcast_to(jnp.arange(TOKENS), (EXPERTS, TOKENS)), axis=1, independent=True)
    log_experts = sum(1 for power in range(1, 20) if EXPERTS >= 2 ** power)
    band_lift = TOKENS + (log_experts * 45426) // LOGIT_MULT
    int_score = (column_perm + chosen * band_lift) * LOGIT_MULT
    return jnp.transpose(int_score).astype(jnp.float32) * (2.0 ** -16)


def setup_inputs(seed: int = 0, part: int = 0) -> dict:
    base_key = jax.random.key(seed)
    k_rows, k_route = jax.random.split(jax.random.fold_in(base_key, part))
    k_in, k_out, k_sin, k_sout = jax.random.split(base_key, 4)
    x_rows = jax.random.normal(k_rows, (TOKENS, D_MODEL), jnp.float32).astype(jnp.bfloat16)
    logits = draw_logits(k_route)
    w_in = (jax.random.normal(k_in, (EXPERTS, D_MODEL, FF_EXPERT), jnp.float32) * D_MODEL ** -0.5).astype(jnp.bfloat16)
    w_out = (jax.random.normal(k_out, (EXPERTS, FF_EXPERT, D_MODEL), jnp.float32) * FF_EXPERT ** -0.5).astype(jnp.bfloat16)
    shared_in = (jax.random.normal(k_sin, (D_MODEL, FF_SHARED), jnp.float32) * D_MODEL ** -0.5).astype(jnp.bfloat16)
    shared_out = (jax.random.normal(k_sout, (FF_SHARED, D_MODEL), jnp.float32) * FF_SHARED ** -0.5).astype(jnp.bfloat16)
    return {"x_rows": x_rows, "logits": logits, "w_in": w_in, "w_out": w_out, "shared_in": shared_in, "shared_out": shared_out}


def reference(x_rows, logits, w_in, w_out, shared_in, shared_out):
    gate_probs = jax.nn.softmax(logits, axis=-1)
    chosen_idx = lax.top_k(logits.T, CAPACITY)[1]

    def expert_step(routed_acc, per_expert):
        tok_idx, gate_col, w_a, w_b = per_expert
        sel_rows = jnp.take(x_rows, tok_idx, axis=0)
        hidden = jax.nn.gelu(jnp.dot(sel_rows, w_a, preferred_element_type=jnp.float32)).astype(jnp.bfloat16)
        expert_out = jnp.dot(hidden, w_b, preferred_element_type=jnp.float32).astype(jnp.bfloat16)
        gate_sel = jnp.take(gate_col, tok_idx)
        routed_acc = routed_acc.at[tok_idx].add(gate_sel[:, None] * expert_out.astype(jnp.float32))
        return routed_acc, None

    routed, _ = lax.scan(expert_step, jnp.zeros((TOKENS, D_MODEL), jnp.float32), (chosen_idx, gate_probs.T, w_in, w_out))
    shared_hidden = jax.nn.gelu(jnp.dot(x_rows, shared_in, preferred_element_type=jnp.float32)).astype(jnp.bfloat16)
    shared_y = jnp.dot(shared_hidden, shared_out, preferred_element_type=jnp.float32).astype(jnp.bfloat16)
    summed = x_rows.astype(jnp.float32) + routed + shared_y.astype(jnp.float32)
    return summed.astype(jnp.bfloat16)
```

```python
import functools

import jax
import jax.numpy as jnp
from jax import lax
from jax.experimental import pallas as pl
from jax.experimental.pallas import tpu as pltpu
from jax.sharding import PartitionSpec as P

CAP_FACTOR = 2
MESH = pl.DeviceIdType.MESH
F32 = jnp.float32
BF16 = jnp.bfloat16
VMEM_BYTES = 64 * 1024 * 1024 - 65536
EXPERT_GROUP = 4


def dot(a, b):
    return jnp.dot(a, b, preferred_element_type=F32)


def gelu(v):
    return jax.nn.gelu(v)


def entry_barrier(me, n):
    barrier = pltpu.get_barrier_semaphore()
    for i in range(1, n):
        pl.semaphore_signal(barrier, inc=1, device_id={"ep": lax.rem(me + i, n)}, device_id_type=MESH)
    pl.semaphore_wait(barrier, n - 1)


def dispatch_kernel(n, chunks, x_hbm, lt_ref, w_hbm, ws_ref, h_ref, hs_ref, route_ref,
                    xb, ltr, scores, probs, pick, xg, hacc, wbuf,
                    x_sem, lt_loc, lt_ss, lt_rs, ss, rs, w_sem):
    me = lax.axis_index("ep")
    core = lax.rem(me, 2)
    partner = me + 1 - 2 * core
    right, left = lax.rem(me + 2, n), lax.rem(me + n - 2, n)
    far = lax.rem(me + 4, n)
    tok_loc, d_model = x_hbm.shape
    num_local, _, ff = w_hbm.shape
    tokens = n * tok_loc
    dc = d_model // chunks
    half = tok_loc // 2
    cap = h_ref.shape[0] // num_local
    groups = num_local // EXPERT_GROUP
    steps = chunks * groups
    depth = wbuf.shape[0]

    def w_copy(step):
        c, g = step // groups, lax.rem(step, groups)
        slot = lax.rem(step, depth)
        return pltpu.make_async_copy(w_hbm.at[pl.ds(g * EXPERT_GROUP, EXPERT_GROUP), pl.ds(c * dc, dc), :], wbuf.at[slot], w_sem.at[slot])

    x_copies = [pltpu.make_async_copy(x_hbm.at[:, pl.ds(c * dc, dc)], xb.at[c, me], x_sem.at[c]) for c in range(chunks)]
    for cp in x_copies:
        cp.start()
    lt_own = pltpu.make_async_copy(lt_ref.at[me], ltr.at[me], lt_loc.at[0])
    lt_own.start()
    for step in range(depth - 1):
        w_copy(step).start()

    entry_barrier(me, n)

    lt_copies = []
    for i in range(1, n):
        dst = lax.rem(me + i, n)
        cp = pltpu.make_async_remote_copy(src_ref=lt_ref.at[dst], dst_ref=ltr.at[me], send_sem=lt_ss.at[i], recv_sem=lt_rs.at[i], device_id={"ep": dst}, device_id_type=MESH)
        cp.start()
        lt_copies.append(cp)

    sent = []

    def send(c, kind, block, rows, to):
        ref = xb.at[c, block] if rows is None else xb.at[c, block, pl.ds(rows, half)]
        cp = pltpu.make_async_remote_copy(src_ref=ref, dst_ref=ref, send_sem=ss.at[c, kind], recv_sem=rs.at[c, kind], device_id={"ep": to}, device_id_type=MESH)
        cp.start()
        sent.append(cp)

    def landed(c, kind, block, rows=None):
        ref = xb.at[c, block] if rows is None else xb.at[c, block, pl.ds(rows, half)]
        pltpu.make_async_remote_copy(src_ref=ref, dst_ref=ref, send_sem=ss.at[c, kind], recv_sem=rs.at[c, kind], device_id={"ep": partner}, device_id_type=MESH).wait_recv()

    def send_own(c):
        x_copies[c].wait()
        send(c, 0, me, None, right)
        send(c, 1, me, None, left)
        send(c, 2, me, None, partner)

    def forward_near(c):
        landed(c, 0, left)
        send(c, 5, left, 0, right)
        send(c, 3, left, None, partner)
        landed(c, 1, right)
        send(c, 6, right, half, left)
        send(c, 4, right, None, partner)

    def forward_far(c):
        landed(c, 5, far, 0)
        send(c, 7, far, 0, partner)
        landed(c, 6, far, half)
        send(c, 8, far, half, partner)

    def flip(d):
        return d + 1 - 2 * core

    def land_partner(c):
        landed(c, 2, partner)
        landed(c, 3, flip(left))
        landed(c, 4, flip(right))
        landed(c, 7, flip(far), 0)
        landed(c, 8, flip(far), half)

    send_own(0)
    if chunks > 1:
        send_own(1)

    @pl.loop(0, tok_loc // 128)
    def _(t):
        rows = pl.ds(pl.multiple_of(t * 128, 128), 128)
        acc = dot(xb[0, me, rows, :], ws_ref[pl.ds(0, dc), :])
        hs_ref[rows, :] = acc

    lt_own.wait()
    for cp in lt_copies:
        cp.wait()
    for s in range(n):
        cols = pl.ds(s * tok_loc, tok_loc)
        block = ltr[s, 0:num_local, :]
        scores[:, cols] = block
        probs[:, cols] = jnp.exp(block - ltr[s, num_local:num_local + 1, :]) / ltr[s, num_local + 1:num_local + 2, :]

    per_row = 128 // cap
    lane = lax.broadcasted_iota(jnp.int32, (num_local, 128), 1)
    home = lax.rem(lax.broadcasted_iota(jnp.int32, (num_local, 128), 0), per_row) * cap
    tok_iota = lax.broadcasted_iota(jnp.int32, (num_local, tokens), 1).astype(F32)

    def extract(j, carry):
        tok_tab, gate_tab = carry
        cur = scores[...]
        top = jnp.max(cur, axis=1, keepdims=True)
        hit = cur == top
        tok = jnp.sum(jnp.where(hit, tok_iota, 0.0), axis=1, keepdims=True)
        gate = jnp.sum(jnp.where(hit, probs[...], 0.0), axis=1, keepdims=True)
        scores[...] = jnp.where(hit, -jnp.inf, cur)
        here = lane == home + j
        return jnp.where(here, tok, tok_tab), jnp.where(here, gate, gate_tab)

    zero = jnp.zeros((num_local, 128), F32)
    tok_tab, gate_tab = lax.fori_loop(0, cap, extract, (zero, zero))
    nrow = num_local // per_row
    tok_rows = [jnp.sum(tok_tab[g * per_row:(g + 1) * per_row], axis=0, keepdims=True) for g in range(nrow)]
    gate_rows = [jnp.sum(gate_tab[g * per_row:(g + 1) * per_row], axis=0, keepdims=True) for g in range(nrow)]
    tok_flat = jnp.concatenate(tok_rows, axis=1)
    gate_flat = jnp.concatenate(gate_rows, axis=1)

    tok_cols = jnp.concatenate(tok_rows, axis=0).T
    for g in range(nrow):
        col = tok_cols[:, g:g + 1]

        @pl.loop(0, n)
        def _(s):
            ids = lax.broadcasted_iota(jnp.int32, (128, tok_loc), 1).astype(F32) + (s * tok_loc).astype(F32)
            pick[pl.ds(g * 128, 128), pl.ds(pl.multiple_of(s * tok_loc, tok_loc), tok_loc)] = jnp.where(ids == col, 1.0, 0.0).astype(BF16)

    rows_total = num_local * cap
    src = jnp.floor(tok_flat * (1.0 / tok_loc))
    loc = tok_flat - src * tok_loc
    of_src = jnp.where(lax.broadcasted_iota(jnp.int32, (n, rows_total), 0).astype(F32) == src, 1.0, 0.0)
    before = jnp.where(lax.broadcasted_iota(jnp.int32, (rows_total, rows_total), 0) < lax.broadcasted_iota(jnp.int32, (rows_total, rows_total), 1), 1.0, 0.0).astype(BF16)
    count = dot(of_src.astype(BF16), before)
    slot = jnp.sum(of_src * count, axis=0, keepdims=True)
    pair_cap = 2 * tok_loc * CAP_FACTOR // n
    hi = jnp.floor(loc * (1.0 / 16))
    g_hi = gate_flat.astype(BF16).astype(F32)
    g_mid = (gate_flat - g_hi).astype(BF16).astype(F32)
    g_lo = gate_flat - g_hi - g_mid
    route_ref[0:1, :] = hi
    route_ref[1:2, :] = loc - 16 * hi
    route_ref[2:3, :] = jnp.ones_like(hi)
    route_ref[3:4, :] = g_hi
    route_ref[4:5, :] = g_mid
    route_ref[5:6, :] = g_lo
    route_ref[6:7, :] = src * pair_cap + slot
    route_ref[7:8, :] = jnp.zeros_like(hi)

    def compute(c):
        @pl.loop(0, rows_total // 256)
        def _(t):
            rows = pl.ds(pl.multiple_of(t * 256, 256), 256)
            acc = dot(pick[rows, 0:tok_loc], xb[c, 0])
            for s in range(1, n):
                acc += dot(pick[rows, s * tok_loc:(s + 1) * tok_loc], xb[c, s])
            xg[rows, :] = acc.astype(BF16)

        @pl.loop(0, groups)
        def _(g):
            step = c * groups + g

            @pl.when(step + depth - 1 < steps)
            def _():
                w_copy(step + depth - 1).start()

            w_copy(step).wait()
            buf = lax.rem(step, depth)
            for i in range(EXPERT_GROUP):
                rows = pl.ds(pl.multiple_of((g * EXPERT_GROUP + i) * cap, cap), cap)
                part = dot(xg[rows, :], wbuf[buf, i])
                hacc[rows, :] = part if c == 0 else hacc[rows, :] + part

    for c in range(chunks):
        forward_near(c)
        if c + 2 < chunks:
            send_own(c + 2)
        if c > 0:
            forward_far(c - 1)
            land_partner(c - 1)
            compute(c - 1)
            @pl.loop(0, tok_loc // 128)
            def _(t):
                rows = pl.ds(pl.multiple_of(t * 128, 128), 128)
                hs_ref[rows, :] += dot(xb[c, me, rows, :], ws_ref[pl.ds(c * dc, dc), :])
    forward_far(chunks - 1)
    land_partner(chunks - 1)
    compute(chunks - 1)

    @pl.loop(0, rows_total // 128)
    def _(t):
        rows = pl.ds(pl.multiple_of(t * 128, 128), 128)
        h_ref[rows, :] = gelu(hacc[rows, :]).astype(BF16)

    for cp in sent:
        cp.wait_send()


def combine_kernel(n, chunks, h_ref, route_ref, w_hbm, x_ref, hs_ref, ws_ref, out_ref,
                   sel, z, sendb, recvb, metas, metar, cmat, hsb, wbuf,
                   m_ss, m_rs, ss, rs, w_sem):
    me = lax.axis_index("ep")
    tok_loc, d_model = x_ref.shape
    num_local, ff, _ = w_hbm.shape
    rows_total = h_ref.shape[0]
    cap = rows_total // num_local
    slots = sel.shape[0]
    pair_cap = slots // n
    dc = d_model // chunks
    groups = num_local // EXPERT_GROUP
    steps = chunks * groups
    depth = wbuf.shape[0]

    def w_copy(step):
        c, g = step // groups, lax.rem(step, groups)
        slot = lax.rem(step, depth)
        return pltpu.make_async_copy(w_hbm.at[pl.ds(g * EXPERT_GROUP, EXPERT_GROUP), :, pl.ds(pl.multiple_of(c * dc, dc), dc)], wbuf.at[slot], w_sem.at[slot])

    for step in range(depth - 1):
        w_copy(step).start()
    entry_barrier(me, n)

    for g in range(rows_total // 128):
        key = route_ref[6:7, g * 128:(g + 1) * 128]

        @pl.loop(0, slots // 256)
        def _(t):
            ids = lax.broadcasted_iota(jnp.int32, (256, 128), 0).astype(F32) + (t * 256).astype(F32)
            sel[pl.ds(pl.multiple_of(t * 256, 256), 256), pl.ds(g * 128, 128)] = jnp.where(ids == key, 1.0, 0.0).astype(BF16)

    vals = route_ref[...].astype(BF16)

    @pl.loop(0, n)
    def _(d):
        block = sel[pl.ds(pl.multiple_of(d * pair_cap, pair_cap), pair_cap), :]
        metas[d] = lax.dot_general(vals, block, (((1,), (1,)), ((), ())), preferred_element_type=F32)

    metar[me] = metas[me]
    meta_copies = []
    for i in range(1, n):
        dst = lax.rem(me + i, n)
        cp = pltpu.make_async_remote_copy(src_ref=metas.at[dst], dst_ref=metar.at[me], send_sem=m_ss.at[i], recv_sem=m_rs.at[i], device_id={"ep": dst}, device_id_type=MESH)
        cp.start()
        meta_copies.append(cp)

    def produce(c):
        @pl.loop(0, groups)
        def _(g):
            step = c * groups + g

            @pl.when(step + depth - 1 < steps)
            def _():
                w_copy(step + depth - 1).start()

            w_copy(step).wait()
            buf = lax.rem(step, depth)
            for i in range(EXPERT_GROUP):
                rows = pl.ds(pl.multiple_of((g * EXPERT_GROUP + i) * cap, cap), cap)
                z[rows, :] = dot(h_ref[rows, :], wbuf[buf, i]).astype(BF16)

        copies = []
        for i in list(range(1, n)) + [0]:
            dst = lax.rem(me + i, n)
            rows = pl.ds(pl.multiple_of(dst * pair_cap, pair_cap), pair_cap)
            mine = pl.ds(pl.multiple_of(me * pair_cap, pair_cap), pair_cap)
            block = dot(sel[rows, :], z[...]).astype(BF16)
            if i == 0:
                recvb[c, mine, :] = block
            else:
                sendb[c, rows, :] = block
                cp = pltpu.make_async_remote_copy(src_ref=sendb.at[c, rows], dst_ref=recvb.at[c, mine], send_sem=ss.at[c, i], recv_sem=rs.at[c, i], device_id={"ep": dst}, device_id_type=MESH)
                cp.start()
                copies.append(cp)
        return copies

    def build_weights():
        for cp in meta_copies:
            cp.wait()

        @pl.loop(0, n)
        def _(o):
            hi, lo, valid = metar[o, 0:1, :], metar[o, 1:2, :], metar[o, 2:3, :]
            tok = 16.0 * hi + lo + valid - 1.0
            ids = lax.broadcasted_iota(jnp.int32, (tok_loc, pair_cap), 0).astype(F32)
            hit = ids == tok
            for k in range(3):
                part = jnp.where(hit, metar[o, 3 + k:4 + k, :], 0.0).astype(BF16)
                cmat[k, :, pl.ds(pl.multiple_of(o * pair_cap, pair_cap), pair_cap)] = part

        hsb[...] = gelu(hs_ref[...]).astype(BF16)

    def finish(c, copies):
        for cp in copies:
            cp.wait()

        @pl.loop(0, tok_loc // 128)
        def _(t):
            rows = pl.ds(pl.multiple_of(t * 128, 128), 128)
            acc = dot(cmat[0, rows, :], recvb[c])
            acc += dot(cmat[1, rows, :], recvb[c])
            acc += dot(cmat[2, rows, :], recvb[c])
            cols = slice(c * dc, (c + 1) * dc)
            shared = dot(hsb[rows, :], ws_ref[:, cols]).astype(BF16).astype(F32)
            out_ref[rows, cols] = (x_ref[rows, cols].astype(F32) + (acc + shared)).astype(BF16)

    pending = produce(0)
    build_weights()
    for c in range(1, chunks):
        nxt = produce(c)
        finish(c - 1, pending)
        pending = nxt
    finish(chunks - 1, pending)


def solution(mesh):
    n = mesh.shape["ep"]
    chunks_a, chunks_b, depth = 4, 4, 4

    def local_layer(x_rows, logits, w_in, w_out, shared_in, shared_out):
        tok_loc, d_model = x_rows.shape
        experts = logits.shape[1]
        num_local = experts // n
        cap = tok_loc * n * CAP_FACTOR // experts
        pair_cap = 2 * tok_loc * CAP_FACTOR // n
        ff = w_in.shape[2]
        tokens, rows_total, slots = n * tok_loc, num_local * cap, n * pair_cap
        dca, dcb = d_model // chunks_a, d_model // chunks_b

        top = jnp.max(logits, axis=1)
        total = jnp.sum(jnp.exp(logits - top[:, None]), axis=1)
        stats = jnp.stack([top, total] + [jnp.zeros_like(top)] * 6)
        lt = jnp.concatenate([logits.T.reshape(n, num_local, tok_loc), jnp.broadcast_to(stats, (n, 8, tok_loc))], axis=1)

        vmem = pl.BlockSpec(memory_space=pltpu.VMEM)
        hbm = pl.BlockSpec(memory_space=pl.ANY)
        dma = pltpu.SemaphoreType.DMA
        h, hs, route = pl.pallas_call(
            functools.partial(dispatch_kernel, n, chunks_a),
            out_shape=[jax.ShapeDtypeStruct((rows_total, ff), BF16), jax.ShapeDtypeStruct((tok_loc, ff), F32), jax.ShapeDtypeStruct((8, rows_total), F32)],
            in_specs=[hbm, vmem, hbm, vmem],
            out_specs=[vmem, vmem, vmem],
            scratch_shapes=[
                pltpu.VMEM((chunks_a, n, tok_loc, dca), BF16),
                pltpu.VMEM((n, num_local + 8, tok_loc), F32),
                pltpu.VMEM((num_local, tokens), F32),
                pltpu.VMEM((num_local, tokens), F32),
                pltpu.VMEM((rows_total, tokens), BF16),
                pltpu.VMEM((rows_total, dca), BF16),
                pltpu.VMEM((rows_total, ff), F32),
                pltpu.VMEM((depth, EXPERT_GROUP, dca, ff), BF16),
                dma((chunks_a,)), dma((1,)), dma((n,)), dma((n,)),
                dma((chunks_a, 9)), dma((chunks_a, 9)), dma((depth,)),
            ],
            compiler_params=pltpu.CompilerParams(collective_id=0, has_side_effects=True, vmem_limit_bytes=VMEM_BYTES),
            name="dispatch",
        )(x_rows, lt, w_in, shared_in)

        return pl.pallas_call(
            functools.partial(combine_kernel, n, chunks_b),
            out_shape=jax.ShapeDtypeStruct((tok_loc, d_model), BF16),
            in_specs=[vmem, vmem, hbm, vmem, vmem, vmem],
            out_specs=vmem,
            scratch_shapes=[
                pltpu.VMEM((slots, rows_total), BF16),
                pltpu.VMEM((rows_total, dcb), BF16),
                pltpu.VMEM((chunks_b, slots, dcb), BF16),
                pltpu.VMEM((chunks_b, slots, dcb), BF16),
                pltpu.VMEM((n, 8, pair_cap), F32),
                pltpu.VMEM((n, 8, pair_cap), F32),
                pltpu.VMEM((3, tok_loc, slots), BF16),
                pltpu.VMEM((tok_loc, shared_in.shape[1]), BF16),
                pltpu.VMEM((depth, EXPERT_GROUP, ff, dcb), BF16),
                dma((n,)), dma((n,)), dma((chunks_b, n)), dma((chunks_b, n)), dma((depth,)),
            ],
            compiler_params=pltpu.CompilerParams(collective_id=1, has_side_effects=True, vmem_limit_bytes=VMEM_BYTES),
            name="combine",
        )(h, route, w_out, x_rows, hs, shared_out)

    row_spec = P(("dp", "ep"), None)
    expert_spec = P("ep", None, None)
    return jax.shard_map(local_layer, mesh=mesh, in_specs=(row_spec, row_spec, expert_spec, expert_spec, P(None, None), P(None, None)), out_specs=row_spec, check_vma=False)
```

```python
import functools

import jax
import jax.numpy as jnp
from jax import lax
from jax.experimental import pallas as pl
from jax.experimental.pallas import tpu as pltpu
from jax.sharding import PartitionSpec as P

CAP_FACTOR = 2
MESH = pl.DeviceIdType.MESH
F32 = jnp.float32
BF16 = jnp.bfloat16
VMEM_BYTES = 64 * 1024 * 1024 - 65536
EXPERT_GROUP = 4
UNIT = 256
SEND_SLOTS = 3
W1_DEPTH = 4
W2_DEPTH = 8
KINDS = 9


def dot(a, b):
    return jnp.dot(a, b, preferred_element_type=F32)


def gelu(v):
    return jax.nn.gelu(v)


def tile(i, size):
    return pl.ds(pl.multiple_of(i * size, size), size)


def layer_kernel(n, x_hbm, lg_hbm, w1_hbm, ws1_hbm, w2_hbm, ws2_hbm, out_hbm,
                 xb, pick, sel, sendb, recvb, xg, hacc, w1buf, w2buf, z, h, hsb, ws1, ws2, stage,
                 sc, gate_p, cand, cand_t, cand_r, m_sc, m_tok, m_gate, route, metas, metar,
                 x_sem, in_sem, c_ss, c_rs, ss, rs, w1_sem, w2_sem, m_ss, m_rs, a_ss, a_rs, o_sem):
    me = lax.axis_index("ep")
    core = lax.rem(me, 2)
    partner = me + 1 - 2 * core
    right, left = lax.rem(me + 2, n), lax.rem(me + n - 2, n)
    far = lax.rem(me + 4, n)
    tok_loc, d_model = x_hbm.shape
    num_local, _, ff = w1_hbm.shape
    nu = d_model // UNIT
    half = tok_loc // 2
    rows_total = hacc.shape[0]
    cap = rows_total // num_local
    slots = sel.shape[0]
    pair_cap = slots // n
    groups = num_local // EXPERT_GROUP
    steps = nu * groups

    def flip(d):
        return d + 1 - 2 * core

    def w1_copy(step):
        u, g, slot = step // groups, lax.rem(step, groups), lax.rem(step, W1_DEPTH)
        return pltpu.make_async_copy(w1_hbm.at[tile(g, EXPERT_GROUP), tile(u, UNIT), :], w1buf.at[slot], w1_sem.at[slot])

    def w2_copy(step):
        u, g, slot = step // groups, lax.rem(step, groups), lax.rem(step, W2_DEPTH)
        return pltpu.make_async_copy(w2_hbm.at[tile(g, EXPERT_GROUP), :, tile(u, UNIT)], w2buf.at[slot], w2_sem.at[slot])

    own = tile(me, tok_loc)
    x_copies = [pltpu.make_async_copy(x_hbm.at[:, pl.ds(u * UNIT, UNIT)], xb.at[u, own], x_sem.at[u]) for u in range(nu)]
    lg_copy = pltpu.make_async_copy(lg_hbm, sc, in_sem.at[0])
    ws1_copy = pltpu.make_async_copy(ws1_hbm, ws1, in_sem.at[1])
    ws2_copy = pltpu.make_async_copy(ws2_hbm, ws2, in_sem.at[2])
    for cp in x_copies + [lg_copy, ws1_copy]:
        cp.start()
    barrier = pltpu.get_barrier_semaphore()
    for i in range(1, n):
        pl.semaphore_signal(barrier, inc=1, device_id={"ep": lax.rem(me + i, n)}, device_id_type=MESH)
    for step in range(W1_DEPTH - 1):
        w1_copy(step).start()
    for cp in x_copies:
        cp.wait()
    pl.semaphore_wait(barrier, n - 1)

    def hop(u, kind, block, part, to):
        rows = tile(block, tok_loc) if part is None else tile(2 * block + part, half)
        ref = xb.at[u, rows]
        return pltpu.make_async_remote_copy(src_ref=ref, dst_ref=ref, send_sem=ss.at[u, kind], recv_sem=rs.at[u, kind], device_id={"ep": to}, device_id_type=MESH)

    def send_own(u):
        hop(u, 0, me, None, right).start()
        hop(u, 1, me, None, left).start()
        hop(u, 2, me, None, partner).start()

    def forward_near(u):
        hop(u, 0, left, None, partner).wait_recv()
        hop(u, 5, left, 0, right).start()
        hop(u, 3, left, None, partner).start()
        hop(u, 1, right, None, partner).wait_recv()
        hop(u, 6, right, 1, left).start()
        hop(u, 4, right, None, partner).start()

    def forward_far(u):
        hop(u, 5, far, 0, partner).wait_recv()
        hop(u, 7, far, 0, partner).start()
        hop(u, 6, far, 1, partner).wait_recv()
        hop(u, 8, far, 1, partner).start()

    def land_partner(u):
        hop(u, 2, partner, None, partner).wait_recv()
        hop(u, 3, flip(left), None, partner).wait_recv()
        hop(u, 4, flip(right), None, partner).wait_recv()
        hop(u, 7, flip(far), 0, partner).wait_recv()
        hop(u, 8, flip(far), 1, partner).wait_recv()

    send_own(0)
    send_own(1)

    lg_copy.wait()
    ws2_copy.start()
    raw = sc[...]
    ex = jnp.exp(raw - jnp.max(raw, axis=1, keepdims=True))
    gate_p[...] = ex / jnp.sum(ex, axis=1, keepdims=True)
    cand[...] = jnp.zeros_like(cand)
    tok_iota = lax.broadcasted_iota(jnp.int32, sc.shape, 0).astype(F32)

    @pl.loop(0, cap)
    def _(j):
        cur = sc[...]
        top = jnp.max(cur, axis=0, keepdims=True)
        hit = cur == top
        cand[pl.ds(j, 1), :] = top
        cand[pl.ds(cap + j, 1), :] = jnp.sum(jnp.where(hit, tok_iota, 0.0), axis=0, keepdims=True)
        cand[pl.ds(2 * cap + j, 1), :] = jnp.sum(jnp.where(hit, gate_p[...], 0.0), axis=0, keepdims=True)
        sc[...] = jnp.where(hit, -jnp.inf, cur)

    flat_t = cand[...].T
    for d in range(n):
        cand_t[d] = flat_t[d * num_local:(d + 1) * num_local]
    cand_r[me] = cand_t[me]
    cand_copies = []
    for i in range(1, n):
        dst = lax.rem(me + i, n)
        cp = pltpu.make_async_remote_copy(src_ref=cand_t.at[dst], dst_ref=cand_r.at[me], send_sem=c_ss.at[i], recv_sem=c_rs.at[i], device_id={"ep": dst}, device_id_type=MESH)
        cp.start()
        cand_copies.append(cp)

    forward_near(0)
    send_own(2)

    ws1_copy.wait()

    @pl.loop(0, tok_loc // 128)
    def _(t):
        rows = pl.ds(pl.multiple_of(me * tok_loc + t * 128, 128), 128)
        acc = dot(xb[0, rows, :], ws1[0:UNIT, :])
        for u in range(1, nu):
            acc += dot(xb[u, rows, :], ws1[u * UNIT:(u + 1) * UNIT, :])
        hsb[tile(t, 128), :] = gelu(acc).astype(BF16)

    forward_near(1)
    send_own(3)

    for cp in cand_copies:
        cp.wait()
    lane = lax.broadcasted_iota(jnp.int32, (num_local, 128), 1)
    for s in range(n):
        block = cand_r[s]
        m_sc[s] = jnp.where(lane < cap, block, -jnp.inf)
        m_tok[s] = pltpu.roll(block, 128 - cap, 1) + float(s) * tok_loc
        m_gate[s] = pltpu.roll(block, 128 - 2 * cap, 1)

    per_row = 128 // cap
    home = lax.rem(lax.broadcasted_iota(jnp.int32, (num_local, 128), 0), per_row) * cap

    def extract(j, carry):
        tok_tab, gate_tab = carry
        cur = m_sc[...]
        top = jnp.max(jnp.max(cur, axis=0), axis=1, keepdims=True)
        hit = cur == top[None]
        tok = jnp.sum(jnp.sum(jnp.where(hit, m_tok[...], 0.0), axis=0), axis=1, keepdims=True)
        gate = jnp.sum(jnp.sum(jnp.where(hit, m_gate[...], 0.0), axis=0), axis=1, keepdims=True)
        m_sc[...] = jnp.where(hit, -jnp.inf, cur)
        here = lane == home + j
        return jnp.where(here, tok, tok_tab), jnp.where(here, gate, gate_tab)

    zero = jnp.zeros((num_local, 128), F32)
    tok_tab, gate_tab = lax.fori_loop(0, cap, extract, (zero, zero))
    nrow = num_local // per_row
    tok_rows = [jnp.sum(tok_tab[g * per_row:(g + 1) * per_row], axis=0, keepdims=True) for g in range(nrow)]
    gate_rows = [jnp.sum(gate_tab[g * per_row:(g + 1) * per_row], axis=0, keepdims=True) for g in range(nrow)]
    tok_flat = jnp.concatenate(tok_rows, axis=1)
    gate_flat = jnp.concatenate(gate_rows, axis=1)

    tok_cols = jnp.concatenate(tok_rows, axis=0).T
    for g in range(nrow):
        col = tok_cols[:, g:g + 1]

        @pl.loop(0, n)
        def _(s):
            ids = lax.broadcasted_iota(jnp.int32, (128, tok_loc), 1).astype(F32) + (s * tok_loc).astype(F32)
            pick[pl.ds(g * 128, 128), tile(s, tok_loc)] = jnp.where(ids == col, 1.0, 0.0).astype(BF16)

    source = jnp.floor(tok_flat * (1.0 / tok_loc))
    loc = tok_flat - source * tok_loc
    of_src = jnp.where(lax.broadcasted_iota(jnp.int32, (n, rows_total), 0).astype(F32) == source, 1.0, 0.0)
    sq = (rows_total, rows_total)
    before = jnp.where(lax.broadcasted_iota(jnp.int32, sq, 0) < lax.broadcasted_iota(jnp.int32, sq, 1), 1.0, 0.0).astype(BF16)
    slot = jnp.sum(of_src * dot(of_src.astype(BF16), before), axis=0, keepdims=True)
    hi = jnp.floor(loc * (1.0 / 16))
    g_hi = gate_flat.astype(BF16).astype(F32)
    g_mid = (gate_flat - g_hi).astype(BF16).astype(F32)
    route[0:1, :] = hi
    route[1:2, :] = loc - 16 * hi
    route[2:3, :] = jnp.ones_like(hi)
    route[3:4, :] = g_hi
    route[4:5, :] = g_mid
    route[5:6, :] = gate_flat - g_hi - g_mid
    route[6:7, :] = source * pair_cap + slot
    route[7:8, :] = jnp.zeros_like(hi)

    def meta_copy(i):
        dst = lax.rem(me + i, n)
        return pltpu.make_async_remote_copy(src_ref=metas.at[dst], dst_ref=metar.at[me], send_sem=m_ss.at[i], recv_sem=m_rs.at[i], device_id={"ep": dst}, device_id_type=MESH)

    def announce():
        for g in range(rows_total // 128):
            key = route[6:7, g * 128:(g + 1) * 128]

            @pl.loop(0, slots // 256)
            def _(t):
                ids = lax.broadcasted_iota(jnp.int32, (256, 128), 0).astype(F32) + (t * 256).astype(F32)
                sel[tile(t, 256), pl.ds(g * 128, 128)] = jnp.where(ids == key, 1.0, 0.0).astype(BF16)

        vals = route[...].astype(BF16)

        @pl.loop(0, n)
        def _(d):
            metas[d] = lax.dot_general(vals, sel[tile(d, pair_cap), :], (((1,), (1,)), ((), ())), preferred_element_type=F32)

        metar[me] = metas[me]
        for i in range(1, n):
            meta_copy(i).start()

    hacc[...] = jnp.zeros_like(hacc)

    def gather(u):
        @pl.loop(0, rows_total // 256)
        def _(t):
            xg[tile(t, 256), :] = dot(pick[tile(t, 256), :], xb[u]).astype(BF16)

    def first_product(u):
        @pl.loop(0, groups)
        def _(g):
            step = u * groups + g

            @pl.when(step + W1_DEPTH - 1 < steps)
            def _():
                w1_copy(step + W1_DEPTH - 1).start()

            w1_copy(step).wait()
            buf = lax.rem(step, W1_DEPTH)
            for i in range(EXPERT_GROUP):
                rows = tile(g * EXPERT_GROUP + i, cap)
                hacc[rows, :] += dot(xg[rows, :], w1buf[buf, i])

    forward_far(0)

    @pl.loop(2, nu + 2)
    def _(u):
        @pl.when(u < nu)
        def _():
            forward_near(u)

        @pl.when(u + 2 < nu)
        def _():
            send_own(u + 2)

        @pl.when(u == 4)
        def _():
            announce()

        land_partner(u - 2)
        gather(u - 2)

        @pl.when(u - 1 < nu)
        def _():
            forward_far(u - 1)

        @pl.when(u == nu)
        def _():
            for step in range(W2_DEPTH - 1):
                w2_copy(step).start()

        first_product(u - 2)

    @pl.loop(0, rows_total // 128)
    def _(t):
        h[tile(t, 128), :] = gelu(hacc[tile(t, 128), :]).astype(BF16)

    def back(u, i):
        dst = lax.rem(me + i, n)
        return pltpu.make_async_remote_copy(src_ref=sendb.at[lax.rem(u, SEND_SLOTS), tile(dst, pair_cap)], dst_ref=recvb.at[u, tile(me, pair_cap)], send_sem=a_ss.at[u, i], recv_sem=a_rs.at[u, i], device_id={"ep": dst}, device_id_type=MESH)

    def produce(u):
        @pl.loop(0, groups)
        def _(g):
            step = u * groups + g

            @pl.when(step + W2_DEPTH - 1 < steps)
            def _():
                w2_copy(step + W2_DEPTH - 1).start()

            w2_copy(step).wait()
            buf = lax.rem(step, W2_DEPTH)
            for i in range(EXPERT_GROUP):
                rows = tile(g * EXPERT_GROUP + i, cap)
                z[rows, :] = dot(h[rows, :], w2buf[buf, i]).astype(BF16)

        @pl.when(u >= SEND_SLOTS)
        def _():
            for i in range(1, n):
                back(u - SEND_SLOTS, i).wait_send()

        @pl.loop(1, n)
        def _(i):
            rows = tile(lax.rem(me + i, n), pair_cap)
            sendb[lax.rem(u, SEND_SLOTS), rows, :] = dot(sel[rows, :], z[...]).astype(BF16)
            back(u, i).start()

        recvb[u, tile(me, pair_cap), :] = dot(sel[tile(me, pair_cap), :], z[...]).astype(BF16)

    def weights_at(k):
        return (tok_loc if k == 1 else 0), (slots if k == 2 else 0)

    def build_weights():
        for i in range(1, n):
            meta_copy(i).wait()

        @pl.loop(0, n)
        def _(o):
            tok = 16.0 * metar[o, 0:1, :] + metar[o, 1:2, :] + metar[o, 2:3, :] - 1.0
            hit = lax.broadcasted_iota(jnp.int32, (tok_loc, pair_cap), 0).astype(F32) == tok
            for k in range(3):
                r0, c0 = weights_at(k)
                pick[pl.ds(r0, tok_loc), pl.ds(pl.multiple_of(c0 + o * pair_cap, pair_cap), pair_cap)] = jnp.where(hit, metar[o, 3 + k:4 + k, :], 0.0).astype(BF16)

    def out_copy(u):
        return pltpu.make_async_copy(stage.at[lax.rem(u, 2)], out_hbm.at[:, tile(u, UNIT)], o_sem.at[lax.rem(u, 2)])

    def finish(u):
        for i in range(1, n):
            back(u, i).wait_recv()

        @pl.when(u >= 2)
        def _():
            out_copy(u - 2).wait()

        @pl.loop(0, tok_loc // 128)
        def _(t):
            acc = jnp.zeros((128, UNIT), F32)
            for k in range(3):
                r0, c0 = weights_at(k)
                acc += dot(pick[pl.ds(pl.multiple_of(r0 + t * 128, 128), 128), c0:c0 + slots], recvb[u])
            shared = dot(hsb[tile(t, 128), :], ws2[:, tile(u, UNIT)]).astype(BF16).astype(F32)
            x_own = xb[u, pl.ds(pl.multiple_of(me * tok_loc + t * 128, 128), 128), :].astype(F32)
            stage[lax.rem(u, 2), tile(t, 128), :] = (x_own + (acc + shared)).astype(BF16)

        out_copy(u).start()

    produce(0)
    build_weights()
    ws2_copy.wait()

    @pl.loop(1, nu)
    def _(u):
        produce(u)
        finish(u - 1)

    finish(nu - 1)
    out_copy(nu - 2).wait()
    out_copy(nu - 1).wait()

    @pl.loop(nu - SEND_SLOTS, nu)
    def _(u):
        for i in range(1, n):
            back(u, i).wait_send()

    @pl.loop(0, nu)
    def _(u):
        hop(u, 0, me, None, right).wait_send()
        hop(u, 1, me, None, left).wait_send()
        hop(u, 2, me, None, partner).wait_send()
        hop(u, 3, left, None, partner).wait_send()
        hop(u, 4, right, None, partner).wait_send()
        hop(u, 5, left, 0, right).wait_send()
        hop(u, 6, right, 1, left).wait_send()
        hop(u, 7, far, 0, partner).wait_send()
        hop(u, 8, far, 1, partner).wait_send()


def solution(mesh):
    n = mesh.shape["ep"]

    def local_layer(x_rows, logits, w_in, w_out, shared_in, shared_out):
        tok_loc, d_model = x_rows.shape
        experts = logits.shape[1]
        num_local = experts // n
        cap = tok_loc * n * CAP_FACTOR // experts
        pair_cap = 2 * tok_loc * CAP_FACTOR // n
        ff = w_in.shape[2]
        tokens, rows_total, slots = n * tok_loc, num_local * cap, n * pair_cap
        nu = d_model // UNIT
        hbm = pl.BlockSpec(memory_space=pl.ANY)
        dma = pltpu.SemaphoreType.DMA
        vmem = pltpu.VMEM
        return pl.pallas_call(
            functools.partial(layer_kernel, n),
            out_shape=jax.ShapeDtypeStruct((tok_loc, d_model), BF16),
            in_specs=[hbm] * 6,
            out_specs=hbm,
            scratch_shapes=[
                vmem((nu, tokens, UNIT), BF16),
                vmem((rows_total, tokens), BF16),
                vmem((slots, rows_total), BF16),
                vmem((SEND_SLOTS, slots, UNIT), BF16),
                vmem((nu, slots, UNIT), BF16),
                vmem((rows_total, UNIT), BF16),
                vmem((rows_total, ff), F32),
                vmem((W1_DEPTH, EXPERT_GROUP, UNIT, ff), BF16),
                vmem((W2_DEPTH, EXPERT_GROUP, ff, UNIT), BF16),
                vmem((rows_total, UNIT), BF16),
                vmem((rows_total, ff), BF16),
                vmem((tok_loc, shared_in.shape[1]), BF16),
                vmem(shared_in.shape, BF16),
                vmem(shared_out.shape, BF16),
                vmem((2, tok_loc, UNIT), BF16),
                vmem((tok_loc, experts), F32),
                vmem((tok_loc, experts), F32),
                vmem((128, experts), F32),
                vmem((n, num_local, 128), F32),
                vmem((n, num_local, 128), F32),
                vmem((n, num_local, 128), F32),
                vmem((n, num_local, 128), F32),
                vmem((n, num_local, 128), F32),
                vmem((8, rows_total), F32),
                vmem((n, 8, pair_cap), F32),
                vmem((n, 8, pair_cap), F32),
                dma((nu,)), dma((3,)), dma((n,)), dma((n,)), dma((nu, KINDS)), dma((nu, KINDS)),
                dma((W1_DEPTH,)), dma((W2_DEPTH,)), dma((n,)), dma((n,)), dma((nu, n)), dma((nu, n)), dma((2,)),
            ],
            compiler_params=pltpu.CompilerParams(collective_id=0, has_side_effects=True, vmem_limit_bytes=VMEM_BYTES),
            name="moe_layer",
        )(x_rows, logits, w_in, shared_in, w_out, shared_out)

    row_spec = P(("dp", "ep"), None)
    expert_spec = P("ep", None, None)
    return jax.shard_map(local_layer, mesh=mesh, in_specs=(row_spec, row_spec, expert_spec, expert_spec, P(None, None), P(None, None)), out_specs=row_spec, check_vma=False)
```

```python
import functools

import jax
import jax.numpy as jnp
from jax import lax
from jax.experimental import pallas as pl
from jax.experimental.pallas import tpu as pltpu
from jax.sharding import PartitionSpec as P

CAP_FACTOR = 2
MESH = pl.DeviceIdType.MESH
F32 = jnp.float32
BF16 = jnp.bfloat16
VMEM_BYTES = 64 * 1024 * 1024 - 65536
EXPERT_GROUP = 4
UNIT = 256
SEND_SLOTS = 3
W1_DEPTH = 6
W2_DEPTH = 8
KINDS = 9


def dot(a, b):
    return jnp.dot(a, b, preferred_element_type=F32)


def gelu(v):
    return jax.nn.gelu(v)


def tile(i, size):
    return pl.ds(pl.multiple_of(i * size, size), size)


def layer_kernel(n, x_hbm, lg_hbm, w1_hbm, ws1_hbm, w2_hbm, ws2_hbm, out_hbm,
                 xb, pick, sel, sendb, xg, hacc, w1buf, w2buf, z, h, hsb, ws1, ws2, stage,
                 sc, gate_p, cand, cand_t, cand_r, m_sc, m_tok, m_gate, route, metas, metar,
                 x_sem, in_sem, c_ss, c_rs, ss, rs, w1_sem, w2_sem, m_ss, m_rs, a_ss, a_rs, o_sem, free_sem):
    me = lax.axis_index("ep")
    core = lax.rem(me, 2)
    partner = me + 1 - 2 * core
    right, left = lax.rem(me + 2, n), lax.rem(me + n - 2, n)
    far = lax.rem(me + 4, n)
    tok_loc, d_model = x_hbm.shape
    num_local, _, ff = w1_hbm.shape
    nu = d_model // UNIT
    half = tok_loc // 2
    rows_total = hacc.shape[0]
    cap = rows_total // num_local
    slots = sel.shape[0]
    pair_cap = slots // n
    groups = num_local // EXPERT_GROUP
    steps = nu * groups

    def flip(d):
        return d + 1 - 2 * core

    def w1_copy(step):
        u, g, slot = step // groups, lax.rem(step, groups), lax.rem(step, W1_DEPTH)
        return pltpu.make_async_copy(w1_hbm.at[tile(g, EXPERT_GROUP), tile(u, UNIT), :], w1buf.at[slot], w1_sem.at[slot])

    def w2_copy(step):
        u, g, slot = step // groups, lax.rem(step, groups), lax.rem(step, W2_DEPTH)
        return pltpu.make_async_copy(w2_hbm.at[tile(g, EXPERT_GROUP), :, tile(u, UNIT)], w2buf.at[slot], w2_sem.at[slot])

    own = tile(me, tok_loc)
    x_copies = [pltpu.make_async_copy(x_hbm.at[:, pl.ds(u * UNIT, UNIT)], xb.at[u, own], x_sem.at[u]) for u in range(nu)]
    lg_copy = pltpu.make_async_copy(lg_hbm, sc, in_sem.at[0])
    ws1_copy = pltpu.make_async_copy(ws1_hbm, ws1, in_sem.at[1])
    ws2_copy = pltpu.make_async_copy(ws2_hbm, ws2, in_sem.at[2])
    for cp in x_copies + [lg_copy, ws1_copy]:
        cp.start()
    barrier = pltpu.get_barrier_semaphore()
    for i in range(1, n):
        pl.semaphore_signal(barrier, inc=1, device_id={"ep": lax.rem(me + i, n)}, device_id_type=MESH)
    for step in range(W1_DEPTH - 1):
        w1_copy(step).start()
    for step in range(W2_DEPTH - 1):
        w2_copy(step).start()
    for cp in x_copies:
        cp.wait()
    pl.semaphore_wait(barrier, n - 1)

    def hop(u, kind, block, part, to):
        rows = tile(block, tok_loc) if part is None else tile(2 * block + part, half)
        ref = xb.at[u, rows]
        return pltpu.make_async_remote_copy(src_ref=ref, dst_ref=ref, send_sem=ss.at[u, kind], recv_sem=rs.at[u, kind], device_id={"ep": to}, device_id_type=MESH)

    def send_own(u):
        hop(u, 0, me, None, right).start()
        hop(u, 1, me, None, left).start()
        hop(u, 2, me, None, partner).start()

    def forward_near(u):
        hop(u, 0, left, None, partner).wait_recv()
        hop(u, 5, left, 0, right).start()
        hop(u, 3, left, None, partner).start()
        hop(u, 1, right, None, partner).wait_recv()
        hop(u, 6, right, 1, left).start()
        hop(u, 4, right, None, partner).start()

    def forward_far(u):
        hop(u, 5, far, 0, partner).wait_recv()
        hop(u, 7, far, 0, partner).start()
        hop(u, 6, far, 1, partner).wait_recv()
        hop(u, 8, far, 1, partner).start()

    def land_near(u):
        hop(u, 2, partner, None, partner).wait_recv()
        hop(u, 3, flip(left), None, partner).wait_recv()
        hop(u, 4, flip(right), None, partner).wait_recv()

    def land_far(u):
        hop(u, 7, flip(far), 0, partner).wait_recv()
        hop(u, 8, flip(far), 1, partner).wait_recv()

    send_own(0)
    send_own(1)

    lg_copy.wait()
    ws2_copy.start()
    raw = sc[...]
    ex = jnp.exp(raw - jnp.max(raw, axis=1, keepdims=True))
    gate_p[...] = ex / jnp.sum(ex, axis=1, keepdims=True)
    cand[...] = jnp.zeros_like(cand)
    tok_iota = lax.broadcasted_iota(jnp.int32, sc.shape, 0).astype(F32)

    @pl.loop(0, cap)
    def _(j):
        cur = sc[...]
        top = jnp.max(cur, axis=0, keepdims=True)
        hit = cur == top
        cand[pl.ds(j, 1), :] = top
        cand[pl.ds(cap + j, 1), :] = jnp.sum(jnp.where(hit, tok_iota, 0.0), axis=0, keepdims=True)
        cand[pl.ds(2 * cap + j, 1), :] = jnp.sum(jnp.where(hit, gate_p[...], 0.0), axis=0, keepdims=True)
        sc[...] = jnp.where(hit, -jnp.inf, cur)

    flat_t = cand[...].T
    for d in range(n):
        cand_t[d] = flat_t[d * num_local:(d + 1) * num_local]
    cand_r[me] = cand_t[me]
    cand_copies = []
    for i in range(1, n):
        dst = lax.rem(me + i, n)
        cp = pltpu.make_async_remote_copy(src_ref=cand_t.at[dst], dst_ref=cand_r.at[me], send_sem=c_ss.at[i], recv_sem=c_rs.at[i], device_id={"ep": dst}, device_id_type=MESH)
        cp.start()
        cand_copies.append(cp)

    forward_near(0)
    send_own(2)

    ws1_copy.wait()

    @pl.loop(0, tok_loc // 128)
    def _(t):
        rows = pl.ds(pl.multiple_of(me * tok_loc + t * 128, 128), 128)
        acc = dot(xb[0, rows, :], ws1[0:UNIT, :])
        for u in range(1, nu):
            acc += dot(xb[u, rows, :], ws1[u * UNIT:(u + 1) * UNIT, :])
        hsb[tile(t, 128), :] = gelu(acc).astype(BF16)

    forward_near(1)
    send_own(3)

    for cp in cand_copies:
        cp.wait()
    lane = lax.broadcasted_iota(jnp.int32, (num_local, 128), 1)
    for s in range(n):
        block = cand_r[s]
        m_sc[s] = jnp.where(lane < cap, block, -jnp.inf)
        m_tok[s] = pltpu.roll(block, 128 - cap, 1) + float(s) * tok_loc
        m_gate[s] = pltpu.roll(block, 128 - 2 * cap, 1)

    per_row = 128 // cap
    home = lax.rem(lax.broadcasted_iota(jnp.int32, (num_local, 128), 0), per_row) * cap

    def extract(j, carry):
        tok_tab, gate_tab = carry
        cur = m_sc[...]
        top = jnp.max(jnp.max(cur, axis=0), axis=1, keepdims=True)
        hit = cur == top[None]
        tok = jnp.sum(jnp.sum(jnp.where(hit, m_tok[...], 0.0), axis=0), axis=1, keepdims=True)
        gate = jnp.sum(jnp.sum(jnp.where(hit, m_gate[...], 0.0), axis=0), axis=1, keepdims=True)
        m_sc[...] = jnp.where(hit, -jnp.inf, cur)
        here = lane == home + j
        return jnp.where(here, tok, tok_tab), jnp.where(here, gate, gate_tab)

    zero = jnp.zeros((num_local, 128), F32)
    tok_tab, gate_tab = lax.fori_loop(0, cap, extract, (zero, zero))
    nrow = num_local // per_row
    tok_rows = [jnp.sum(tok_tab[g * per_row:(g + 1) * per_row], axis=0, keepdims=True) for g in range(nrow)]
    gate_rows = [jnp.sum(gate_tab[g * per_row:(g + 1) * per_row], axis=0, keepdims=True) for g in range(nrow)]
    tok_flat = jnp.concatenate(tok_rows, axis=1)
    gate_flat = jnp.concatenate(gate_rows, axis=1)

    tok_cols = jnp.concatenate(tok_rows, axis=0).T
    for g in range(nrow):
        col = tok_cols[:, g:g + 1]

        @pl.loop(0, n)
        def _(s):
            ids = lax.broadcasted_iota(jnp.int32, (128, tok_loc), 1).astype(F32) + (s * tok_loc).astype(F32)
            pick[pl.ds(g * 128, 128), tile(s, tok_loc)] = jnp.where(ids == col, 1.0, 0.0).astype(BF16)

    source = jnp.floor(tok_flat * (1.0 / tok_loc))
    loc = tok_flat - source * tok_loc
    of_src = jnp.where(lax.broadcasted_iota(jnp.int32, (n, rows_total), 0).astype(F32) == source, 1.0, 0.0)
    sq = (rows_total, rows_total)
    before = jnp.where(lax.broadcasted_iota(jnp.int32, sq, 0) < lax.broadcasted_iota(jnp.int32, sq, 1), 1.0, 0.0).astype(BF16)
    slot = jnp.sum(of_src * dot(of_src.astype(BF16), before), axis=0, keepdims=True)
    hi = jnp.floor(loc * (1.0 / 16))
    g_hi = gate_flat.astype(BF16).astype(F32)
    g_mid = (gate_flat - g_hi).astype(BF16).astype(F32)
    route[0:1, :] = hi
    route[1:2, :] = loc - 16 * hi
    route[2:3, :] = jnp.ones_like(hi)
    route[3:4, :] = g_hi
    route[4:5, :] = g_mid
    route[5:6, :] = gate_flat - g_hi - g_mid
    route[6:7, :] = source * pair_cap + slot
    route[7:8, :] = jnp.zeros_like(hi)

    def meta_copy(i):
        dst = lax.rem(me + i, n)
        return pltpu.make_async_remote_copy(src_ref=metas.at[dst], dst_ref=metar.at[me], send_sem=m_ss.at[i], recv_sem=m_rs.at[i], device_id={"ep": dst}, device_id_type=MESH)

    def announce():
        for g in range(rows_total // 128):
            key = route[6:7, g * 128:(g + 1) * 128]

            @pl.loop(0, slots // 256)
            def _(t):
                ids = lax.broadcasted_iota(jnp.int32, (256, 128), 0).astype(F32) + (t * 256).astype(F32)
                sel[tile(t, 256), pl.ds(g * 128, 128)] = jnp.where(ids == key, 1.0, 0.0).astype(BF16)

        vals = route[...].astype(BF16)

        @pl.loop(0, n)
        def _(d):
            metas[d] = lax.dot_general(vals, sel[tile(d, pair_cap), :], (((1,), (1,)), ((), ())), preferred_element_type=F32)

        metar[me] = metas[me]
        for i in range(1, n):
            meta_copy(i).start()

    hacc[...] = jnp.zeros_like(hacc)
    chip = 2 * tok_loc
    near_chips = [lax.rem(me // 2 + k, n // 2) for k in (0, 1, n // 2 - 1)]
    far_chip = far // 2

    def gather_near(u):
        land_near(u)

        @pl.loop(0, rows_total // 256)
        def _(t):
            acc = dot(pick[tile(t, 256), tile(near_chips[0], chip)], xb[u, tile(near_chips[0], chip), :])
            for q in near_chips[1:]:
                acc += dot(pick[tile(t, 256), tile(q, chip)], xb[u, tile(q, chip), :])
            xg[lax.rem(u, 2), tile(t, 256), :] = acc.astype(BF16)

    def gather_far(u):
        land_far(u)

        @pl.loop(0, rows_total // 256)
        def _(t):
            acc = dot(pick[tile(t, 256), tile(far_chip, chip)], xb[u, tile(far_chip, chip), :])
            xg[lax.rem(u, 2), tile(t, 256), :] = (xg[lax.rem(u, 2), tile(t, 256), :].astype(F32) + acc).astype(BF16)

    def next_w1(step):
        @pl.when(step + W1_DEPTH - 1 < steps)
        def _():
            w1_copy(step + W1_DEPTH - 1).start()

        w1_copy(step).wait()
        return lax.rem(step, W1_DEPTH)

    def next_w2(step):
        @pl.when(step + W2_DEPTH - 1 < steps)
        def _():
            w2_copy(step + W2_DEPTH - 1).start()

        w2_copy(step).wait()
        return lax.rem(step, W2_DEPTH)

    def first_product(u, lo, hi_):
        @pl.loop(lo, hi_)
        def _(g):
            buf = next_w1(u * groups + g)
            for i in range(EXPERT_GROUP):
                rows = tile(g * EXPERT_GROUP + i, cap)
                hacc[rows, :] += dot(xg[lax.rem(u, 2), rows, :], w1buf[buf, i])

    forward_far(0)

    @pl.loop(2, 4)
    def _(u):
        forward_near(u)
        send_own(u + 2)
        gather_near(u - 2)
        gather_far(u - 2)
        forward_far(u - 1)
        first_product(u - 2, 0, groups)

    @pl.loop(4, nu)
    def _(u):
        forward_near(u)

        @pl.when(u + 2 < nu)
        def _():
            send_own(u + 2)

        @pl.when(u == 4)
        def _():
            gather_near(2)
            gather_far(2)
            first_product(2, 0, groups)
            announce()
            gather_near(3)

        gather_near(u)
        forward_far(u - 1)
        gather_far(u - 1)
        first_product(u - 1, 0, groups // 2)

        @pl.when(u == nu - 1)
        def _():
            forward_far(nu - 1)

        first_product(u - 1, groups // 2, groups)

    gather_far(nu - 1)

    @pl.loop(0, nu)
    def _(u):
        hop(u, 0, me, None, right).wait_send()
        hop(u, 1, me, None, left).wait_send()
        hop(u, 2, me, None, partner).wait_send()
        hop(u, 3, left, None, partner).wait_send()
        hop(u, 4, right, None, partner).wait_send()
        hop(u, 5, left, 0, right).wait_send()
        hop(u, 6, right, 1, left).wait_send()
        hop(u, 7, far, 0, partner).wait_send()
        hop(u, 8, far, 1, partner).wait_send()

    for i in range(1, n):
        pl.semaphore_signal(free_sem, inc=1, device_id={"ep": lax.rem(me + i, n)}, device_id_type=MESH)

    @pl.loop(0, groups)
    def _(g):
        buf1, buf2 = next_w1((nu - 1) * groups + g), next_w2(g)
        for i in range(EXPERT_GROUP):
            rows = tile(g * EXPERT_GROUP + i, cap)
            act = gelu(hacc[rows, :] + dot(xg[(nu - 1) % 2, rows, :], w1buf[buf1, i])).astype(BF16)
            h[rows, :] = act
            z[rows, :] = dot(act, w2buf[buf2, i]).astype(BF16)

    pl.semaphore_wait(free_sem, n - 1)

    def landing(d):
        return (n // 2) * tok_loc * (1 - d // (n // 2))

    def back(u, i):
        dst = lax.rem(me + i, n)
        return pltpu.make_async_remote_copy(src_ref=sendb.at[lax.rem(u, SEND_SLOTS), tile(dst, pair_cap)], dst_ref=xb.at[u, pl.ds(pl.multiple_of(landing(dst) + me * pair_cap, pair_cap), pair_cap)], send_sem=a_ss.at[u, i], recv_sem=a_rs.at[u, i], device_id={"ep": dst}, device_id_type=MESH)

    def arrived(u, i):
        src = lax.rem(me + n - i, n)
        ref = xb.at[u, pl.ds(pl.multiple_of(landing(me) + src * pair_cap, pair_cap), pair_cap)]
        pltpu.make_async_remote_copy(src_ref=ref, dst_ref=ref, send_sem=a_ss.at[u, i], recv_sem=a_rs.at[u, i], device_id={"ep": partner}, device_id_type=MESH).wait_recv()

    def second_product(u):
        @pl.loop(0, groups)
        def _(g):
            buf = next_w2(u * groups + g)
            for i in range(EXPERT_GROUP):
                rows = tile(g * EXPERT_GROUP + i, cap)
                z[rows, :] = dot(h[rows, :], w2buf[buf, i]).astype(BF16)

    def send_back(u):
        @pl.when(u >= SEND_SLOTS)
        def _():
            for i in range(1, n):
                back(u - SEND_SLOTS, i).wait_send()

        @pl.loop(1, n)
        def _(i):
            rows = tile(lax.rem(me + i, n), pair_cap)
            sendb[lax.rem(u, SEND_SLOTS), rows, :] = dot(sel[rows, :], z[...]).astype(BF16)
            back(u, i).start()

        xb[u, pl.ds(pl.multiple_of(landing(me) + me * pair_cap, pair_cap), pair_cap), :] = dot(sel[tile(me, pair_cap), :], z[...]).astype(BF16)

    def weights_at(k):
        return (tok_loc if k == 1 else 0), (slots if k == 2 else 0)

    def build_weights():
        for i in range(1, n):
            meta_copy(i).wait()

        @pl.loop(0, n)
        def _(o):
            tok = 16.0 * metar[o, 0:1, :] + metar[o, 1:2, :] + metar[o, 2:3, :] - 1.0
            hit = lax.broadcasted_iota(jnp.int32, (tok_loc, pair_cap), 0).astype(F32) == tok
            for k in range(3):
                r0, c0 = weights_at(k)
                pick[pl.ds(r0, tok_loc), pl.ds(pl.multiple_of(c0 + o * pair_cap, pair_cap), pair_cap)] = jnp.where(hit, metar[o, 3 + k:4 + k, :], 0.0).astype(BF16)

    def out_copy(u):
        return pltpu.make_async_copy(stage.at[lax.rem(u, 2)], out_hbm.at[:, tile(u, UNIT)], o_sem.at[lax.rem(u, 2)])

    def finish(u):
        @pl.when(u >= 2)
        def _():
            out_copy(u - 2).wait()

        pair = 2 * pair_cap
        for k, q in enumerate(near_chips + [far_chip]):
            if k == 0:
                arrived(u, lax.rem(me + n - partner, n))
            else:
                arrived(u, lax.rem(me + n - 2 * q, n))
                arrived(u, lax.rem(me + n - 2 * q - 1 + n, n))

            @pl.loop(0, tok_loc // 128)
            def _(t):
                rows = tile(t, 128)
                got = xb[u, pl.ds(pl.multiple_of(landing(me) + q * pair, pair), pair), :]
                acc = hacc[rows, 0:UNIT] if k > 0 else dot(hsb[rows, :], ws2[:, tile(u, UNIT)]).astype(BF16).astype(F32)
                for part in range(3):
                    r0, c0 = weights_at(part)
                    acc += dot(pick[pl.ds(pl.multiple_of(r0 + t * 128, 128), 128), pl.ds(pl.multiple_of(c0 + q * pair, pair), pair)], got)
                if k < 3:
                    hacc[rows, 0:UNIT] = acc
                else:
                    x_own = xb[u, pl.ds(pl.multiple_of(me * tok_loc + t * 128, 128), 128), :].astype(F32)
                    stage[lax.rem(u, 2), rows, :] = (x_own + acc).astype(BF16)

        out_copy(u).start()

    send_back(0)
    build_weights()
    ws2_copy.wait()

    @pl.loop(1, nu)
    def _(u):
        second_product(u)
        send_back(u)
        finish(u - 1)

    finish(nu - 1)
    out_copy(nu - 2).wait()
    out_copy(nu - 1).wait()

    @pl.loop(nu - SEND_SLOTS, nu)
    def _(u):
        for i in range(1, n):
            back(u, i).wait_send()


def solution(mesh):
    n = mesh.shape["ep"]

    def local_layer(x_rows, logits, w_in, w_out, shared_in, shared_out):
        tok_loc, d_model = x_rows.shape
        experts = logits.shape[1]
        num_local = experts // n
        cap = tok_loc * n * CAP_FACTOR // experts
        pair_cap = 2 * tok_loc * CAP_FACTOR // n
        ff = w_in.shape[2]
        tokens, rows_total, slots = n * tok_loc, num_local * cap, n * pair_cap
        nu = d_model // UNIT
        hbm = pl.BlockSpec(memory_space=pl.ANY)
        dma = pltpu.SemaphoreType.DMA
        vmem = pltpu.VMEM
        return pl.pallas_call(
            functools.partial(layer_kernel, n),
            out_shape=jax.ShapeDtypeStruct((tok_loc, d_model), BF16),
            in_specs=[hbm] * 6,
            out_specs=hbm,
            scratch_shapes=[
                vmem((nu, tokens, UNIT), BF16),
                vmem((rows_total, tokens), BF16),
                vmem((slots, rows_total), BF16),
                vmem((SEND_SLOTS, slots, UNIT), BF16),
                vmem((2, rows_total, UNIT), BF16),
                vmem((rows_total, ff), F32),
                vmem((W1_DEPTH, EXPERT_GROUP, UNIT, ff), BF16),
                vmem((W2_DEPTH, EXPERT_GROUP, ff, UNIT), BF16),
                vmem((rows_total, UNIT), BF16),
                vmem((rows_total, ff), BF16),
                vmem((tok_loc, shared_in.shape[1]), BF16),
                vmem(shared_in.shape, BF16),
                vmem(shared_out.shape, BF16),
                vmem((2, tok_loc, UNIT), BF16),
                vmem((tok_loc, experts), F32),
                vmem((tok_loc, experts), F32),
                vmem((128, experts), F32),
                vmem((n, num_local, 128), F32),
                vmem((n, num_local, 128), F32),
                vmem((n, num_local, 128), F32),
                vmem((n, num_local, 128), F32),
                vmem((n, num_local, 128), F32),
                vmem((8, rows_total), F32),
                vmem((n, 8, pair_cap), F32),
                vmem((n, 8, pair_cap), F32),
                dma((nu,)), dma((3,)), dma((n,)), dma((n,)), dma((nu, KINDS)), dma((nu, KINDS)),
                dma((W1_DEPTH,)), dma((W2_DEPTH,)), dma((n,)), dma((n,)), dma((nu, n)), dma((nu, n)), dma((2,)), pltpu.SemaphoreType.REGULAR,
            ],
            compiler_params=pltpu.CompilerParams(collective_id=0, has_side_effects=True, vmem_limit_bytes=VMEM_BYTES),
            name="moe_layer",
        )(x_rows, logits, w_in, shared_in, w_out, shared_out)

    row_spec = P(("dp", "ep"), None)
    expert_spec = P("ep", None, None)
    return jax.shard_map(local_layer, mesh=mesh, in_specs=(row_spec, row_spec, expert_spec, expert_spec, P(None, None), P(None, None)), out_specs=row_spec, check_vma=False)
```

```python
import functools

import jax
import jax.numpy as jnp
from jax import lax
from jax.experimental import pallas as pl
from jax.experimental.pallas import tpu as pltpu
from jax.sharding import PartitionSpec as P

CAP_FACTOR = 2
MESH = pl.DeviceIdType.MESH
F32 = jnp.float32
BF16 = jnp.bfloat16
VMEM_BYTES = 64 * 1024 * 1024 - 65536
EXPERT_GROUP = 4
UNIT = 256
SEND_SLOTS = 3
W1_DEPTH = 6
W2_DEPTH = 8
KINDS = 9
GATHER_ROWS = 512


def dot(a, b):
    return jnp.dot(a, b, preferred_element_type=F32)


def gelu(v):
    return jax.nn.gelu(v)


def tile(i, size):
    return pl.ds(pl.multiple_of(i * size, size), size)


def layer_kernel(n, x_hbm, lg_hbm, w1_hbm, ws1_hbm, w2_hbm, ws2_hbm, out_hbm,
                 xb, pick, sel, sendb, xg, hacc, w1buf, w2buf, z, h, hsb, ws1, ws2, stage,
                 sc, gate_p, cand, cand_t, cand_r, m_sc, m_tok, m_gate, route, metas, metar,
                 x_sem, in_sem, c_ss, c_rs, ss, rs, w1_sem, w2_sem, m_ss, m_rs, a_ss, a_rs, o_sem, free_sem):
    me = lax.axis_index("ep")
    core = lax.rem(me, 2)
    partner = me + 1 - 2 * core
    right, left = lax.rem(me + 2, n), lax.rem(me + n - 2, n)
    far = lax.rem(me + 4, n)
    tok_loc, d_model = x_hbm.shape
    num_local, _, ff = w1_hbm.shape
    nu = d_model // UNIT
    half = tok_loc // 2
    rows_total = hacc.shape[0]
    cap = rows_total // num_local
    slots = sel.shape[0]
    pair_cap = slots // n
    groups = num_local // EXPERT_GROUP
    steps = nu * groups

    def flip(d):
        return d + 1 - 2 * core

    def w1_copy(step):
        u, g, slot = step // groups, lax.rem(step, groups), lax.rem(step, W1_DEPTH)
        return pltpu.make_async_copy(w1_hbm.at[tile(g, EXPERT_GROUP), tile(u, UNIT), :], w1buf.at[slot], w1_sem.at[slot])

    def w2_copy(step):
        u, g, slot = step // groups, lax.rem(step, groups), lax.rem(step, W2_DEPTH)
        return pltpu.make_async_copy(w2_hbm.at[tile(g, EXPERT_GROUP), :, tile(u, UNIT)], w2buf.at[slot], w2_sem.at[slot])

    own = tile(me, tok_loc)
    x_copies = [pltpu.make_async_copy(x_hbm.at[:, pl.ds(u * UNIT, UNIT)], xb.at[u, own], x_sem.at[u]) for u in range(nu)]
    lg_copy = pltpu.make_async_copy(lg_hbm, sc, in_sem.at[0])
    ws1_copy = pltpu.make_async_copy(ws1_hbm, ws1, in_sem.at[1])
    ws2_copy = pltpu.make_async_copy(ws2_hbm, ws2, in_sem.at[2])
    for cp in x_copies + [lg_copy, ws1_copy]:
        cp.start()
    barrier = pltpu.get_barrier_semaphore()
    for i in range(1, n):
        pl.semaphore_signal(barrier, inc=1, device_id={"ep": lax.rem(me + i, n)}, device_id_type=MESH)
    for cp in x_copies:
        cp.wait()
    pl.semaphore_wait(barrier, n - 1)

    def hop(u, kind, block, part, to):
        rows = tile(block, tok_loc) if part is None else tile(2 * block + part, half)
        ref = xb.at[u, rows]
        return pltpu.make_async_remote_copy(src_ref=ref, dst_ref=ref, send_sem=ss.at[u, kind], recv_sem=rs.at[u, kind], device_id={"ep": to}, device_id_type=MESH)

    def send_own(u):
        hop(u, 0, me, None, right).start()
        hop(u, 1, me, None, left).start()
        hop(u, 2, me, None, partner).start()

    def forward_near(u):
        hop(u, 0, left, None, partner).wait_recv()
        hop(u, 5, left, 0, right).start()
        hop(u, 3, left, None, partner).start()
        hop(u, 1, right, None, partner).wait_recv()
        hop(u, 6, right, 1, left).start()
        hop(u, 4, right, None, partner).start()

    def forward_far(u):
        hop(u, 5, far, 0, partner).wait_recv()
        hop(u, 7, far, 0, partner).start()
        hop(u, 6, far, 1, partner).wait_recv()
        hop(u, 8, far, 1, partner).start()

    def land_near(u):
        hop(u, 2, partner, None, partner).wait_recv()
        hop(u, 3, flip(left), None, partner).wait_recv()
        hop(u, 4, flip(right), None, partner).wait_recv()

    def land_far(u):
        hop(u, 7, flip(far), 0, partner).wait_recv()
        hop(u, 8, flip(far), 1, partner).wait_recv()

    send_own(0)
    send_own(1)
    for step in range(W1_DEPTH - 1):
        w1_copy(step).start()
    for step in range(W2_DEPTH - 1):
        w2_copy(step).start()

    lg_copy.wait()
    ws2_copy.start()
    raw = sc[...]
    ex = jnp.exp(raw - jnp.max(raw, axis=1, keepdims=True))
    gate_p[...] = ex / jnp.sum(ex, axis=1, keepdims=True)
    cand[...] = jnp.zeros_like(cand)
    tok_iota = lax.broadcasted_iota(jnp.int32, sc.shape, 0).astype(F32)

    @pl.loop(0, cap)
    def _(j):
        cur = sc[...]
        top = jnp.max(cur, axis=0, keepdims=True)
        hit = cur == top
        cand[pl.ds(j, 1), :] = top
        cand[pl.ds(cap + j, 1), :] = jnp.sum(jnp.where(hit, tok_iota, 0.0), axis=0, keepdims=True)
        cand[pl.ds(2 * cap + j, 1), :] = jnp.sum(jnp.where(hit, gate_p[...], 0.0), axis=0, keepdims=True)
        sc[...] = jnp.where(hit, -jnp.inf, cur)

    flat_t = cand[...].T
    for d in range(n):
        cand_t[d] = flat_t[d * num_local:(d + 1) * num_local]
    cand_r[me] = cand_t[me]
    cand_copies = []
    for i in range(1, n):
        dst = lax.rem(me + i, n)
        cp = pltpu.make_async_remote_copy(src_ref=cand_t.at[dst], dst_ref=cand_r.at[me], send_sem=c_ss.at[i], recv_sem=c_rs.at[i], device_id={"ep": dst}, device_id_type=MESH)
        cp.start()
        cand_copies.append(cp)

    forward_near(0)
    send_own(2)

    forward_near(1)
    send_own(3)

    for cp in cand_copies:
        cp.wait()
    lane = lax.broadcasted_iota(jnp.int32, (num_local, 128), 1)
    for s in range(n):
        block = cand_r[s]
        m_sc[s] = jnp.where(lane < cap, block, -jnp.inf)
        m_tok[s] = pltpu.roll(block, 128 - cap, 1) + float(s) * tok_loc
        m_gate[s] = pltpu.roll(block, 128 - 2 * cap, 1)

    per_row = 128 // cap
    home = lax.rem(lax.broadcasted_iota(jnp.int32, (num_local, 128), 0), per_row) * cap

    def extract(j, carry):
        tok_tab, gate_tab = carry
        cur = m_sc[...]
        top = jnp.max(jnp.max(cur, axis=0), axis=1, keepdims=True)
        hit = cur == top[None]
        tok = jnp.sum(jnp.sum(jnp.where(hit, m_tok[...], 0.0), axis=0), axis=1, keepdims=True)
        gate = jnp.sum(jnp.sum(jnp.where(hit, m_gate[...], 0.0), axis=0), axis=1, keepdims=True)
        m_sc[...] = jnp.where(hit, -jnp.inf, cur)
        here = lane == home + j
        return jnp.where(here, tok, tok_tab), jnp.where(here, gate, gate_tab)

    zero = jnp.zeros((num_local, 128), F32)
    tok_tab, gate_tab = lax.fori_loop(0, cap, extract, (zero, zero))
    nrow = num_local // per_row
    tok_rows = [jnp.sum(tok_tab[g * per_row:(g + 1) * per_row], axis=0, keepdims=True) for g in range(nrow)]
    gate_rows = [jnp.sum(gate_tab[g * per_row:(g + 1) * per_row], axis=0, keepdims=True) for g in range(nrow)]
    tok_flat = jnp.concatenate(tok_rows, axis=1)
    gate_flat = jnp.concatenate(gate_rows, axis=1)

    tok_cols = jnp.concatenate(tok_rows, axis=0).T
    for g in range(nrow):
        col = tok_cols[:, g:g + 1]

        @pl.loop(0, n)
        def _(s):
            ids = lax.broadcasted_iota(jnp.int32, (128, tok_loc), 1).astype(F32) + (s * tok_loc).astype(F32)
            pick[pl.ds(g * 128, 128), tile(s, tok_loc)] = jnp.where(ids == col, 1.0, 0.0).astype(BF16)

    route[6:7, :] = tok_flat
    route[7:8, :] = gate_flat

    def meta_copy(i):
        dst = lax.rem(me + i, n)
        return pltpu.make_async_remote_copy(src_ref=metas.at[dst], dst_ref=metar.at[me], send_sem=m_ss.at[i], recv_sem=m_rs.at[i], device_id={"ep": dst}, device_id_type=MESH)

    def announce():
        tok_flat, gate_flat = route[6:7, :], route[7:8, :]
        source = jnp.floor(tok_flat * (1.0 / tok_loc))
        loc = tok_flat - source * tok_loc
        of_src = jnp.where(lax.broadcasted_iota(jnp.int32, (n, rows_total), 0).astype(F32) == source, 1.0, 0.0)
        sq = (rows_total, rows_total)
        before = jnp.where(lax.broadcasted_iota(jnp.int32, sq, 0) < lax.broadcasted_iota(jnp.int32, sq, 1), 1.0, 0.0).astype(BF16)
        slot = jnp.sum(of_src * dot(of_src.astype(BF16), before), axis=0, keepdims=True)
        hi = jnp.floor(loc * (1.0 / 16))
        g_hi = gate_flat.astype(BF16).astype(F32)
        g_mid = (gate_flat - g_hi).astype(BF16).astype(F32)
        route[0:1, :] = hi
        route[1:2, :] = loc - 16 * hi
        route[2:3, :] = jnp.ones_like(hi)
        route[3:4, :] = g_hi
        route[4:5, :] = g_mid
        route[5:6, :] = gate_flat - g_hi - g_mid
        route[6:7, :] = source * pair_cap + slot
        route[7:8, :] = jnp.zeros_like(hi)

        for g in range(rows_total // 128):
            key = route[6:7, g * 128:(g + 1) * 128]

            @pl.loop(0, slots // 256)
            def _(t):
                ids = lax.broadcasted_iota(jnp.int32, (256, 128), 0).astype(F32) + (t * 256).astype(F32)
                sel[tile(t, 256), pl.ds(g * 128, 128)] = jnp.where(ids == key, 1.0, 0.0).astype(BF16)

        vals = route[...].astype(BF16)

        @pl.loop(0, n)
        def _(d):
            metas[d] = lax.dot_general(vals, sel[tile(d, pair_cap), :], (((1,), (1,)), ((), ())), preferred_element_type=F32)

        metar[me] = metas[me]
        for i in range(1, n):
            meta_copy(i).start()

    hacc[...] = jnp.zeros_like(hacc)
    chip = 2 * tok_loc
    near_chips = [lax.rem(me // 2 + k, n // 2) for k in (0, 1, n // 2 - 1)]
    far_chip = far // 2

    def gather_near(u):
        land_near(u)

        @pl.loop(0, rows_total // GATHER_ROWS)
        def _(t):
            rows = tile(t, GATHER_ROWS)
            acc = dot(pick[rows, tile(near_chips[0], chip)], xb[u, tile(near_chips[0], chip), :])
            for q in near_chips[1:]:
                acc += dot(pick[rows, tile(q, chip)], xb[u, tile(q, chip), :])
            xg[lax.rem(u, 2), rows, :] = acc.astype(BF16)

    def gather_far(u):
        land_far(u)

        @pl.loop(0, rows_total // GATHER_ROWS)
        def _(t):
            rows = tile(t, GATHER_ROWS)
            acc = dot(pick[rows, tile(far_chip, chip)], xb[u, tile(far_chip, chip), :])
            xg[lax.rem(u, 2), rows, :] = (xg[lax.rem(u, 2), rows, :].astype(F32) + acc).astype(BF16)

    def gather(u):
        land_near(u)
        land_far(u)

        @pl.loop(0, rows_total // GATHER_ROWS)
        def _(t):
            rows = tile(t, GATHER_ROWS)
            xg[lax.rem(u, 2), rows, :] = dot(pick[rows, :], xb[u]).astype(BF16)

    def next_w1(step):
        @pl.when(step + W1_DEPTH - 1 < steps)
        def _():
            w1_copy(step + W1_DEPTH - 1).start()

        w1_copy(step).wait()
        return lax.rem(step, W1_DEPTH)

    def next_w2(step):
        @pl.when(step + W2_DEPTH - 1 < steps)
        def _():
            w2_copy(step + W2_DEPTH - 1).start()

        w2_copy(step).wait()
        return lax.rem(step, W2_DEPTH)

    def first_product(u, lo, hi_):
        @pl.loop(lo, hi_)
        def _(g):
            buf = next_w1(u * groups + g)
            for i in range(EXPERT_GROUP):
                rows = tile(g * EXPERT_GROUP + i, cap)
                hacc[rows, :] += dot(xg[lax.rem(u, 2), rows, :], w1buf[buf, i])

    forward_near(2)
    send_own(4)
    forward_far(0)
    gather(0)
    first_product(0, 0, groups)
    forward_far(1)
    gather(1)

    @pl.loop(3, nu - 1)
    def _(u):
        forward_near(u)

        @pl.when(u + 2 < nu)
        def _():
            send_own(u + 2)

        first_product(u - 2, 0, groups)
        forward_far(u - 1)
        gather(u - 1)

        @pl.when(u == 4)
        def _():
            announce()

    first_product(nu - 3, 0, groups)
    gather_near(nu - 2)
    forward_near(nu - 1)
    forward_far(nu - 2)
    gather_near(nu - 1)
    gather_far(nu - 2)
    forward_far(nu - 1)
    first_product(nu - 2, 0, groups)
    gather_far(nu - 1)

    @pl.loop(0, nu)
    def _(u):
        hop(u, 0, me, None, right).wait_send()
        hop(u, 1, me, None, left).wait_send()
        hop(u, 2, me, None, partner).wait_send()
        hop(u, 3, left, None, partner).wait_send()
        hop(u, 4, right, None, partner).wait_send()
        hop(u, 5, left, 0, right).wait_send()
        hop(u, 6, right, 1, left).wait_send()
        hop(u, 7, far, 0, partner).wait_send()
        hop(u, 8, far, 1, partner).wait_send()

    for i in range(1, n):
        pl.semaphore_signal(free_sem, inc=1, device_id={"ep": lax.rem(me + i, n)}, device_id_type=MESH)

    @pl.loop(0, groups)
    def _(g):
        buf1, buf2 = next_w1((nu - 1) * groups + g), next_w2(g)
        for i in range(EXPERT_GROUP):
            rows = tile(g * EXPERT_GROUP + i, cap)
            act = gelu(hacc[rows, :] + dot(xg[(nu - 1) % 2, rows, :], w1buf[buf1, i])).astype(BF16)
            h[rows, :] = act
            z[rows, :] = dot(act, w2buf[buf2, i]).astype(BF16)

    pl.semaphore_wait(free_sem, n - 1)

    def landing(d):
        return (n // 2) * tok_loc * (1 - d // (n // 2))

    def back(u, i):
        dst = lax.rem(me + i, n)
        return pltpu.make_async_remote_copy(src_ref=sendb.at[lax.rem(u, SEND_SLOTS), tile(dst, pair_cap)], dst_ref=xb.at[u, pl.ds(pl.multiple_of(landing(dst) + me * pair_cap, pair_cap), pair_cap)], send_sem=a_ss.at[u, i], recv_sem=a_rs.at[u, i], device_id={"ep": dst}, device_id_type=MESH)

    def arrived(u, i):
        src = lax.rem(me + n - i, n)
        ref = xb.at[u, pl.ds(pl.multiple_of(landing(me) + src * pair_cap, pair_cap), pair_cap)]
        pltpu.make_async_remote_copy(src_ref=ref, dst_ref=ref, send_sem=a_ss.at[u, i], recv_sem=a_rs.at[u, i], device_id={"ep": partner}, device_id_type=MESH).wait_recv()

    def second_product(u):
        @pl.loop(0, groups)
        def _(g):
            buf = next_w2(u * groups + g)
            for i in range(EXPERT_GROUP):
                rows = tile(g * EXPERT_GROUP + i, cap)
                z[rows, :] = dot(h[rows, :], w2buf[buf, i]).astype(BF16)

    def send_back(u):
        @pl.when(u >= SEND_SLOTS)
        def _():
            for i in range(1, n):
                back(u - SEND_SLOTS, i).wait_send()

        pair = 2 * pair_cap
        chip_me = me // 2

        @pl.loop(1, n // 2)
        def _(k):
            q = lax.rem(chip_me + k, n // 2)
            sendb[lax.rem(u, SEND_SLOTS), tile(q, pair), :] = dot(sel[tile(q, pair), :], z[...]).astype(BF16)
            back(u, lax.rem(2 * q - me + n, n)).start()
            back(u, lax.rem(2 * q + 1 - me + n, n)).start()

        sendb[lax.rem(u, SEND_SLOTS), tile(partner, pair_cap), :] = dot(sel[tile(partner, pair_cap), :], z[...]).astype(BF16)
        back(u, lax.rem(partner - me + n, n)).start()
        xb[u, pl.ds(pl.multiple_of(landing(me) + me * pair_cap, pair_cap), pair_cap), :] = dot(sel[tile(me, pair_cap), :], z[...]).astype(BF16)

    def weights_at(k):
        return (tok_loc if k == 1 else 0), (slots if k == 2 else 0)

    def build_weights():
        for i in range(1, n):
            meta_copy(i).wait()

        @pl.loop(0, n)
        def _(o):
            tok = 16.0 * metar[o, 0:1, :] + metar[o, 1:2, :] + metar[o, 2:3, :] - 1.0
            hit = lax.broadcasted_iota(jnp.int32, (tok_loc, pair_cap), 0).astype(F32) == tok
            for k in range(3):
                r0, c0 = weights_at(k)
                pick[pl.ds(r0, tok_loc), pl.ds(pl.multiple_of(c0 + o * pair_cap, pair_cap), pair_cap)] = jnp.where(hit, metar[o, 3 + k:4 + k, :], 0.0).astype(BF16)

    def out_copy(u):
        return pltpu.make_async_copy(stage.at[lax.rem(u, 2)], out_hbm.at[:, tile(u, UNIT)], o_sem.at[lax.rem(u, 2)])

    def finish(u, last=False):
        @pl.when(u >= 2)
        def _():
            out_copy(u - 2).wait()

        pair = 2 * pair_cap

        def shared(rows):
            return dot(hsb[rows, :], ws2[:, tile(u, UNIT)]).astype(BF16).astype(F32)

        def weighted(t, acc, q):
            for part in range(3):
                r0, c0 = weights_at(part)
                lhs_rows = pl.ds(pl.multiple_of(r0 + t * 128, 128), 128)
                if q is None:
                    acc += dot(pick[lhs_rows, c0:c0 + slots], xb[u, pl.ds(pl.multiple_of(landing(me), slots), slots), :])
                else:
                    acc += dot(pick[lhs_rows, pl.ds(pl.multiple_of(c0 + q * pair, pair), pair)], xb[u, pl.ds(pl.multiple_of(landing(me) + q * pair, pair), pair), :])
            return acc

        def write(t, acc):
            x_own = xb[u, pl.ds(pl.multiple_of(me * tok_loc + t * 128, 128), 128), :].astype(F32)
            stage[lax.rem(u, 2), tile(t, 128), :] = (x_own + acc).astype(BF16)

        def chip_arrived(q):
            arrived(u, lax.rem(me + n - 2 * q, n))
            arrived(u, lax.rem(me + n - 2 * q - 1 + n, n))

        arrived(u, lax.rem(me + n - partner, n))
        chip_arrived(near_chips[1])
        chip_arrived(near_chips[2])
        if last:
            @pl.loop(0, tok_loc // 128)
            def _(t):
                acc = shared(tile(t, 128))
                for q in near_chips:
                    acc = weighted(t, acc, q)
                hacc[tile(t, 128), 0:UNIT] = acc

            chip_arrived(far_chip)

            @pl.loop(0, tok_loc // 128)
            def _(t):
                write(t, weighted(t, hacc[tile(t, 128), 0:UNIT], far_chip))
        else:
            chip_arrived(far_chip)

            @pl.loop(0, tok_loc // 128)
            def _(t):
                write(t, weighted(t, shared(tile(t, 128)), None))

        out_copy(u).start()

    send_back(0)
    build_weights()
    ws1_copy.wait()
    ws2_copy.wait()

    @pl.loop(0, tok_loc // 128)
    def _(t):
        rows = pl.ds(pl.multiple_of(me * tok_loc + t * 128, 128), 128)
        acc = dot(xb[0, rows, :], ws1[0:UNIT, :])
        for u in range(1, nu):
            acc += dot(xb[u, rows, :], ws1[u * UNIT:(u + 1) * UNIT, :])
        hsb[tile(t, 128), :] = gelu(acc).astype(BF16)


    @pl.loop(1, nu)
    def _(u):
        second_product(u)
        send_back(u)
        finish(u - 1)

    finish(nu - 1, True)
    out_copy(nu - 2).wait()
    out_copy(nu - 1).wait()

    @pl.loop(nu - SEND_SLOTS, nu)
    def _(u):
        for i in range(1, n):
            back(u, i).wait_send()


def solution(mesh):
    n = mesh.shape["ep"]

    def local_layer(x_rows, logits, w_in, w_out, shared_in, shared_out):
        tok_loc, d_model = x_rows.shape
        experts = logits.shape[1]
        num_local = experts // n
        cap = tok_loc * n * CAP_FACTOR // experts
        pair_cap = 2 * tok_loc * CAP_FACTOR // n
        ff = w_in.shape[2]
        tokens, rows_total, slots = n * tok_loc, num_local * cap, n * pair_cap
        nu = d_model // UNIT
        hbm = pl.BlockSpec(memory_space=pl.ANY)
        dma = pltpu.SemaphoreType.DMA
        vmem = pltpu.VMEM
        return pl.pallas_call(
            functools.partial(layer_kernel, n),
            out_shape=jax.ShapeDtypeStruct((tok_loc, d_model), BF16),
            in_specs=[hbm] * 6,
            out_specs=hbm,
            scratch_shapes=[
                vmem((nu, tokens, UNIT), BF16),
                vmem((rows_total, tokens), BF16),
                vmem((slots, rows_total), BF16),
                vmem((SEND_SLOTS, slots, UNIT), BF16),
                vmem((2, rows_total, UNIT), BF16),
                vmem((rows_total, ff), F32),
                vmem((W1_DEPTH, EXPERT_GROUP, UNIT, ff), BF16),
                vmem((W2_DEPTH, EXPERT_GROUP, ff, UNIT), BF16),
                vmem((rows_total, UNIT), BF16),
                vmem((rows_total, ff), BF16),
                vmem((tok_loc, shared_in.shape[1]), BF16),
                vmem(shared_in.shape, BF16),
                vmem(shared_out.shape, BF16),
                vmem((2, tok_loc, UNIT), BF16),
                vmem((tok_loc, experts), F32),
                vmem((tok_loc, experts), F32),
                vmem((128, experts), F32),
                vmem((n, num_local, 128), F32),
                vmem((n, num_local, 128), F32),
                vmem((n, num_local, 128), F32),
                vmem((n, num_local, 128), F32),
                vmem((n, num_local, 128), F32),
                vmem((8, rows_total), F32),
                vmem((n, 8, pair_cap), F32),
                vmem((n, 8, pair_cap), F32),
                dma((nu,)), dma((3,)), dma((n,)), dma((n,)), dma((nu, KINDS)), dma((nu, KINDS)),
                dma((W1_DEPTH,)), dma((W2_DEPTH,)), dma((n,)), dma((n,)), dma((nu, n)), dma((nu, n)), dma((2,)), pltpu.SemaphoreType.REGULAR,
            ],
            compiler_params=pltpu.CompilerParams(collective_id=0, has_side_effects=True, vmem_limit_bytes=VMEM_BYTES),
            name="moe_layer",
        )(x_rows, logits, w_in, shared_in, w_out, shared_out)

    row_spec = P(("dp", "ep"), None)
    expert_spec = P("ep", None, None)
    return jax.shard_map(local_layer, mesh=mesh, in_specs=(row_spec, row_spec, expert_spec, expert_spec, P(None, None), P(None, None)), out_specs=row_spec, check_vma=False)
```

```python
import functools

import jax
import jax.numpy as jnp
from jax import lax
from jax.experimental import pallas as pl
from jax.experimental.pallas import tpu as pltpu
from jax.sharding import PartitionSpec as P

CAP_FACTOR = 2
MESH = pl.DeviceIdType.MESH
F32 = jnp.float32
BF16 = jnp.bfloat16
VMEM_BYTES = 60 * 1024 * 1024
EXPERT_GROUP = 8
UNIT = 256
SEND_SLOTS = 3
W1_DEPTH = 4
W2_DEPTH = 4
KINDS = 9
GATHER_ROWS = 512


def dot(a, b):
    return jnp.dot(a, b, preferred_element_type=F32)


def gelu(v):
    return jax.nn.gelu(v)


def tile(i, size):
    return pl.ds(pl.multiple_of(i * size, size), size)


def layer_kernel(n, x_hbm, lg_hbm, w1_hbm, ws1_hbm, w2_hbm, ws2_hbm, out_ref,
                 xb, pick, sel, sendb, xg, hacc, w1buf, w2buf, z, h, hsb, ws1, ws2,
                 sc, gate_p, cand, cand_t, cand_r, m_sc, m_tok, m_gate, route, metas, metar,
                 x_sem, in_sem, c_ss, c_rs, ss, rs, w1_sem, w2_sem, m_ss, m_rs, a_ss, a_rs, free_sem):
    me = lax.axis_index("ep")
    core = lax.rem(me, 2)
    partner = me + 1 - 2 * core
    right, left = lax.rem(me + 2, n), lax.rem(me + n - 2, n)
    far = lax.rem(me + 4, n)
    tok_loc, d_model = x_hbm.shape
    num_local, _, ff = w1_hbm.shape
    nu = d_model // UNIT
    half = tok_loc // 2
    rows_total = hacc.shape[0]
    cap = rows_total // num_local
    slots = sel.shape[0]
    pair_cap = slots // n
    groups = num_local // EXPERT_GROUP
    steps = nu * groups

    def flip(d):
        return d + 1 - 2 * core

    def w1_copy(step):
        u, g, slot = step // groups, lax.rem(step, groups), lax.rem(step, W1_DEPTH)
        return pltpu.make_async_copy(w1_hbm.at[tile(g, EXPERT_GROUP), tile(u, UNIT), :], w1buf.at[slot], w1_sem.at[slot])

    def w2_copy(step):
        u, g, slot = step // groups, lax.rem(step, groups), lax.rem(step, W2_DEPTH)
        return pltpu.make_async_copy(w2_hbm.at[tile(g, EXPERT_GROUP), :, tile(u, UNIT)], w2buf.at[slot], w2_sem.at[slot])

    own = tile(me, tok_loc)
    x_copies = [pltpu.make_async_copy(x_hbm.at[:, pl.ds(u * UNIT, UNIT)], xb.at[u, own], x_sem.at[u]) for u in range(nu)]
    lg_copy = pltpu.make_async_copy(lg_hbm, sc, in_sem.at[0])
    ws1_copy = pltpu.make_async_copy(ws1_hbm, ws1, in_sem.at[1])
    ws2_copy = pltpu.make_async_copy(ws2_hbm, ws2, in_sem.at[2])
    for cp in x_copies + [lg_copy, ws1_copy]:
        cp.start()
    barrier = pltpu.get_barrier_semaphore()
    for i in range(1, n):
        pl.semaphore_signal(barrier, inc=1, device_id={"ep": lax.rem(me + i, n)}, device_id_type=MESH)
    for cp in x_copies:
        cp.wait()
    pl.semaphore_wait(barrier, n - 1)

    def hop(u, kind, block, part, to):
        rows = tile(block, tok_loc) if part is None else tile(2 * block + part, half)
        ref = xb.at[u, rows]
        return pltpu.make_async_remote_copy(src_ref=ref, dst_ref=ref, send_sem=ss.at[u, kind], recv_sem=rs.at[u, kind], device_id={"ep": to}, device_id_type=MESH)

    def send_own(u):
        hop(u, 0, me, None, right).start()
        hop(u, 1, me, None, left).start()
        hop(u, 2, me, None, partner).start()

    def forward_near(u):
        hop(u, 0, left, None, partner).wait_recv()
        hop(u, 5, left, 0, right).start()
        hop(u, 3, left, None, partner).start()
        hop(u, 1, right, None, partner).wait_recv()
        hop(u, 6, right, 1, left).start()
        hop(u, 4, right, None, partner).start()

    def forward_far(u):
        hop(u, 5, far, 0, partner).wait_recv()
        hop(u, 7, far, 0, partner).start()
        hop(u, 6, far, 1, partner).wait_recv()
        hop(u, 8, far, 1, partner).start()

    def land_near(u):
        hop(u, 2, partner, None, partner).wait_recv()
        hop(u, 3, flip(left), None, partner).wait_recv()
        hop(u, 4, flip(right), None, partner).wait_recv()

    def land_far(u):
        hop(u, 7, flip(far), 0, partner).wait_recv()
        hop(u, 8, flip(far), 1, partner).wait_recv()

    send_own(0)
    send_own(1)
    for step in range(W1_DEPTH - 1):
        w1_copy(step).start()
    for step in range(W2_DEPTH - 1):
        w2_copy(step).start()

    lg_copy.wait()
    ws2_copy.start()
    raw = sc[...]
    ex = jnp.exp(raw - jnp.max(raw, axis=1, keepdims=True))
    gate_p[...] = ex / jnp.sum(ex, axis=1, keepdims=True)
    cand[...] = jnp.zeros_like(cand)
    tok_iota = lax.broadcasted_iota(jnp.int32, sc.shape, 0).astype(F32)

    def best_local(j, top):
        cur = sc[...]
        hit = cur == top
        cand[pl.ds(j, 1), :] = top
        cand[pl.ds(cap + j, 1), :] = jnp.sum(jnp.where(hit, tok_iota, 0.0), axis=0, keepdims=True)
        cand[pl.ds(2 * cap + j, 1), :] = jnp.sum(jnp.where(hit, gate_p[...], 0.0), axis=0, keepdims=True)
        cur = jnp.where(hit, -jnp.inf, cur)
        sc[...] = cur
        return jnp.max(cur, axis=0, keepdims=True)

    lax.fori_loop(0, cap, best_local, jnp.max(raw, axis=0, keepdims=True))

    flat_t = cand[...].T
    for d in range(n):
        cand_t[d] = flat_t[d * num_local:(d + 1) * num_local]
    cand_r[me] = cand_t[me]
    cand_copies = []
    for i in range(1, n):
        dst = lax.rem(me + i, n)
        cp = pltpu.make_async_remote_copy(src_ref=cand_t.at[dst], dst_ref=cand_r.at[me], send_sem=c_ss.at[i], recv_sem=c_rs.at[i], device_id={"ep": dst}, device_id_type=MESH)
        cp.start()
        cand_copies.append(cp)

    forward_near(0)
    send_own(2)

    forward_near(1)
    send_own(3)

    for cp in cand_copies:
        cp.wait()
    lane = lax.broadcasted_iota(jnp.int32, (num_local, 128), 1)
    for s in range(n):
        block = cand_r[s]
        m_sc[s] = jnp.where(lane < cap, block, -jnp.inf)
        m_tok[s] = pltpu.roll(block, 128 - cap, 1) + float(s) * tok_loc
        m_gate[s] = pltpu.roll(block, 128 - 2 * cap, 1)

    per_row = 128 // cap
    home = lax.rem(lax.broadcasted_iota(jnp.int32, (num_local, 128), 0), per_row) * cap

    def extract(j, carry):
        tok_tab, gate_tab = carry
        cur = m_sc[...]
        top = jnp.max(jnp.max(cur, axis=0), axis=1, keepdims=True)
        hit = cur == top[None]
        tok = jnp.sum(jnp.sum(jnp.where(hit, m_tok[...], 0.0), axis=0), axis=1, keepdims=True)
        gate = jnp.sum(jnp.sum(jnp.where(hit, m_gate[...], 0.0), axis=0), axis=1, keepdims=True)
        m_sc[...] = jnp.where(hit, -jnp.inf, cur)
        here = lane == home + j
        return jnp.where(here, tok, tok_tab), jnp.where(here, gate, gate_tab)

    zero = jnp.zeros((num_local, 128), F32)
    tok_tab, gate_tab = lax.fori_loop(0, cap, extract, (zero, zero))
    nrow = num_local // per_row
    tok_rows = [jnp.sum(tok_tab[g * per_row:(g + 1) * per_row], axis=0, keepdims=True) for g in range(nrow)]
    gate_rows = [jnp.sum(gate_tab[g * per_row:(g + 1) * per_row], axis=0, keepdims=True) for g in range(nrow)]
    tok_flat = jnp.concatenate(tok_rows, axis=1)
    gate_flat = jnp.concatenate(gate_rows, axis=1)

    tok_cols = jnp.concatenate(tok_rows, axis=0).T
    for g in range(nrow):
        col = tok_cols[:, g:g + 1]

        @pl.loop(0, n)
        def _(s):
            ids = lax.broadcasted_iota(jnp.int32, (128, tok_loc), 1).astype(F32) + (s * tok_loc).astype(F32)
            pick[pl.ds(g * 128, 128), tile(s, tok_loc)] = jnp.where(ids == col, 1.0, 0.0).astype(BF16)

    route[6:7, :] = tok_flat
    route[7:8, :] = gate_flat

    def meta_copy(i):
        dst = lax.rem(me + i, n)
        return pltpu.make_async_remote_copy(src_ref=metas.at[dst], dst_ref=metar.at[me], send_sem=m_ss.at[i], recv_sem=m_rs.at[i], device_id={"ep": dst}, device_id_type=MESH)

    def announce():
        tok_flat, gate_flat = route[6:7, :], route[7:8, :]
        source = jnp.floor(tok_flat * (1.0 / tok_loc))
        loc = tok_flat - source * tok_loc
        of_src = jnp.where(lax.broadcasted_iota(jnp.int32, (n, rows_total), 0).astype(F32) == source, 1.0, 0.0)
        sq = (rows_total, rows_total)
        before = jnp.where(lax.broadcasted_iota(jnp.int32, sq, 0) < lax.broadcasted_iota(jnp.int32, sq, 1), 1.0, 0.0).astype(BF16)
        slot = jnp.sum(of_src * dot(of_src.astype(BF16), before), axis=0, keepdims=True)
        hi = jnp.floor(loc * (1.0 / 16))
        g_hi = gate_flat.astype(BF16).astype(F32)
        g_mid = (gate_flat - g_hi).astype(BF16).astype(F32)
        route[0:1, :] = hi
        route[1:2, :] = loc - 16 * hi
        route[2:3, :] = jnp.ones_like(hi)
        route[3:4, :] = g_hi
        route[4:5, :] = g_mid
        route[5:6, :] = gate_flat - g_hi - g_mid
        route[6:7, :] = source * pair_cap + slot
        route[7:8, :] = jnp.zeros_like(hi)

        for g in range(rows_total // 128):
            key = route[6:7, g * 128:(g + 1) * 128]

            @pl.loop(0, slots // 256)
            def _(t):
                ids = lax.broadcasted_iota(jnp.int32, (256, 128), 0).astype(F32) + (t * 256).astype(F32)
                sel[tile(t, 256), pl.ds(g * 128, 128)] = jnp.where(ids == key, 1.0, 0.0).astype(BF16)

        vals = route[...].astype(BF16)

        @pl.loop(0, n)
        def _(d):
            metas[d] = lax.dot_general(vals, sel[tile(d, pair_cap), :], (((1,), (1,)), ((), ())), preferred_element_type=F32)

        metar[me] = metas[me]
        for i in range(1, n):
            meta_copy(i).start()

    hacc[...] = jnp.zeros_like(hacc)
    chip = 2 * tok_loc
    near_chips = [lax.rem(me // 2 + k, n // 2) for k in (0, 1, n // 2 - 1)]
    far_chip = far // 2

    def gather_near(u):
        land_near(u)

        @pl.loop(0, rows_total // GATHER_ROWS)
        def _(t):
            rows = tile(t, GATHER_ROWS)
            acc = dot(pick[rows, tile(near_chips[0], chip)], xb[u, tile(near_chips[0], chip), :])
            for q in near_chips[1:]:
                acc += dot(pick[rows, tile(q, chip)], xb[u, tile(q, chip), :])
            xg[lax.rem(u, 2), rows, :] = acc.astype(BF16)

    def gather_far(u):
        land_far(u)

        @pl.loop(0, rows_total // GATHER_ROWS)
        def _(t):
            rows = tile(t, GATHER_ROWS)
            acc = dot(pick[rows, tile(far_chip, chip)], xb[u, tile(far_chip, chip), :])
            xg[lax.rem(u, 2), rows, :] = (xg[lax.rem(u, 2), rows, :].astype(F32) + acc).astype(BF16)

    def gather(u):
        land_near(u)
        land_far(u)

        @pl.loop(0, rows_total // GATHER_ROWS)
        def _(t):
            rows = tile(t, GATHER_ROWS)
            xg[lax.rem(u, 2), rows, :] = dot(pick[rows, :], xb[u]).astype(BF16)

    def next_w1(step):
        @pl.when(step + W1_DEPTH - 1 < steps)
        def _():
            w1_copy(step + W1_DEPTH - 1).start()

        w1_copy(step).wait()
        return lax.rem(step, W1_DEPTH)

    def next_w2(step):
        @pl.when(step + W2_DEPTH - 1 < steps)
        def _():
            w2_copy(step + W2_DEPTH - 1).start()

        w2_copy(step).wait()
        return lax.rem(step, W2_DEPTH)

    def first_product(u, lo, hi_):
        @pl.loop(lo, hi_)
        def _(g):
            buf = next_w1(u * groups + g)
            for i in range(EXPERT_GROUP):
                rows = tile(g * EXPERT_GROUP + i, cap)
                hacc[rows, :] += dot(xg[lax.rem(u, 2), rows, :], w1buf[buf, i])

    forward_near(2)
    send_own(4)
    forward_far(0)
    gather(0)
    first_product(0, 0, groups)
    forward_far(1)
    gather(1)

    @pl.loop(3, nu - 1)
    def _(u):
        forward_near(u)

        @pl.when(u + 2 < nu)
        def _():
            send_own(u + 2)

        first_product(u - 2, 0, groups)
        forward_far(u - 1)
        gather(u - 1)

        @pl.when(u == 4)
        def _():
            announce()

    first_product(nu - 3, 0, groups)
    forward_near(nu - 1)
    gather_near(nu - 2)
    forward_far(nu - 2)
    gather_near(nu - 1)
    gather_far(nu - 2)
    forward_far(nu - 1)
    first_product(nu - 2, 0, groups)
    gather_far(nu - 1)

    @pl.loop(0, nu)
    def _(u):
        hop(u, 0, me, None, right).wait_send()
        hop(u, 1, me, None, left).wait_send()
        hop(u, 2, me, None, partner).wait_send()
        hop(u, 3, left, None, partner).wait_send()
        hop(u, 4, right, None, partner).wait_send()
        hop(u, 5, left, 0, right).wait_send()
        hop(u, 6, right, 1, left).wait_send()
        hop(u, 7, far, 0, partner).wait_send()
        hop(u, 8, far, 1, partner).wait_send()

    for i in range(1, n):
        pl.semaphore_signal(free_sem, inc=1, device_id={"ep": lax.rem(me + i, n)}, device_id_type=MESH)

    @pl.loop(0, groups)
    def _(g):
        buf1, buf2 = next_w1((nu - 1) * groups + g), next_w2(g)
        for i in range(EXPERT_GROUP):
            rows = tile(g * EXPERT_GROUP + i, cap)
            act = gelu(hacc[rows, :] + dot(xg[(nu - 1) % 2, rows, :], w1buf[buf1, i])).astype(BF16)
            h[rows, :] = act
            z[rows, :] = dot(act, w2buf[buf2, i]).astype(BF16)

    pl.semaphore_wait(free_sem, n - 1)

    def landing(d):
        return (n // 2) * tok_loc * (1 - d // (n // 2))

    def back(u, i):
        dst = lax.rem(me + i, n)
        return pltpu.make_async_remote_copy(src_ref=sendb.at[lax.rem(u, SEND_SLOTS), tile(dst, pair_cap)], dst_ref=xb.at[u, pl.ds(pl.multiple_of(landing(dst) + me * pair_cap, pair_cap), pair_cap)], send_sem=a_ss.at[u, i], recv_sem=a_rs.at[u, i], device_id={"ep": dst}, device_id_type=MESH)

    def arrived(u, i):
        src = lax.rem(me + n - i, n)
        ref = xb.at[u, pl.ds(pl.multiple_of(landing(me) + src * pair_cap, pair_cap), pair_cap)]
        pltpu.make_async_remote_copy(src_ref=ref, dst_ref=ref, send_sem=a_ss.at[u, i], recv_sem=a_rs.at[u, i], device_id={"ep": partner}, device_id_type=MESH).wait_recv()

    def second_product(u):
        @pl.loop(0, groups)
        def _(g):
            buf = next_w2(u * groups + g)
            for i in range(EXPERT_GROUP):
                rows = tile(g * EXPERT_GROUP + i, cap)
                z[rows, :] = dot(h[rows, :], w2buf[buf, i]).astype(BF16)

    def send_back(u):
        @pl.when(u >= SEND_SLOTS)
        def _():
            for i in range(1, n):
                back(u - SEND_SLOTS, i).wait_send()

        pair = 2 * pair_cap
        chip_me = me // 2

        @pl.loop(1, n // 2)
        def _(k):
            q = lax.rem(chip_me + k, n // 2)
            sendb[lax.rem(u, SEND_SLOTS), tile(q, pair), :] = dot(sel[tile(q, pair), :], z[...]).astype(BF16)
            back(u, lax.rem(2 * q - me + n, n)).start()
            back(u, lax.rem(2 * q + 1 - me + n, n)).start()

        sendb[lax.rem(u, SEND_SLOTS), tile(partner, pair_cap), :] = dot(sel[tile(partner, pair_cap), :], z[...]).astype(BF16)
        back(u, lax.rem(partner - me + n, n)).start()
        xb[u, pl.ds(pl.multiple_of(landing(me) + me * pair_cap, pair_cap), pair_cap), :] = dot(sel[tile(me, pair_cap), :], z[...]).astype(BF16)

    def weights_at(k):
        return (tok_loc if k == 1 else 0), (slots if k == 2 else 0)

    def build_weights():
        for i in range(1, n):
            meta_copy(i).wait()

        @pl.loop(0, n)
        def _(o):
            tok = 16.0 * metar[o, 0:1, :] + metar[o, 1:2, :] + metar[o, 2:3, :] - 1.0
            hit = lax.broadcasted_iota(jnp.int32, (tok_loc, pair_cap), 0).astype(F32) == tok
            for k in range(3):
                r0, c0 = weights_at(k)
                pick[pl.ds(r0, tok_loc), pl.ds(pl.multiple_of(c0 + o * pair_cap, pair_cap), pair_cap)] = jnp.where(hit, metar[o, 3 + k:4 + k, :], 0.0).astype(BF16)

    def finish(u, last=False):
        pair = 2 * pair_cap

        def shared(rows):
            return dot(hsb[rows, :], ws2[:, tile(u, UNIT)]).astype(BF16).astype(F32)

        def weighted(t, acc, q):
            for part in range(3):
                r0, c0 = weights_at(part)
                lhs_rows = pl.ds(pl.multiple_of(r0 + t * 128, 128), 128)
                if q is None:
                    acc += dot(pick[lhs_rows, c0:c0 + slots], xb[u, pl.ds(pl.multiple_of(landing(me), slots), slots), :])
                else:
                    acc += dot(pick[lhs_rows, pl.ds(pl.multiple_of(c0 + q * pair, pair), pair)], xb[u, pl.ds(pl.multiple_of(landing(me) + q * pair, pair), pair), :])
            return acc

        def write(t, acc):
            x_own = xb[u, pl.ds(pl.multiple_of(me * tok_loc + t * 128, 128), 128), :].astype(F32)
            out_ref[tile(t, 128), tile(u, UNIT)] = (x_own + acc).astype(BF16)

        def chip_arrived(q):
            arrived(u, lax.rem(me + n - 2 * q, n))
            arrived(u, lax.rem(me + n - 2 * q - 1 + n, n))

        arrived(u, lax.rem(me + n - partner, n))
        chip_arrived(near_chips[1])
        chip_arrived(near_chips[2])
        if last:
            @pl.loop(0, tok_loc // 128)
            def _(t):
                acc = shared(tile(t, 128))
                for q in near_chips:
                    acc = weighted(t, acc, q)
                hacc[tile(t, 128), 0:UNIT] = acc

            chip_arrived(far_chip)

            @pl.loop(0, tok_loc // 128)
            def _(t):
                write(t, weighted(t, hacc[tile(t, 128), 0:UNIT], far_chip))
        else:
            chip_arrived(far_chip)

            @pl.loop(0, tok_loc // 128)
            def _(t):
                write(t, weighted(t, shared(tile(t, 128)), None))


    send_back(0)
    build_weights()
    ws1_copy.wait()
    ws2_copy.wait()

    @pl.loop(0, tok_loc // 128)
    def _(t):
        rows = pl.ds(pl.multiple_of(me * tok_loc + t * 128, 128), 128)
        acc = dot(xb[0, rows, :], ws1[0:UNIT, :])
        for u in range(1, nu):
            acc += dot(xb[u, rows, :], ws1[u * UNIT:(u + 1) * UNIT, :])
        hsb[tile(t, 128), :] = gelu(acc).astype(BF16)


    @pl.loop(1, nu)
    def _(u):
        second_product(u)
        send_back(u)
        finish(u - 1)

    finish(nu - 1, True)

    @pl.loop(nu - SEND_SLOTS, nu)
    def _(u):
        for i in range(1, n):
            back(u, i).wait_send()


def solution(mesh):
    n = mesh.shape["ep"]

    def local_layer(x_rows, logits, w_in, w_out, shared_in, shared_out):
        tok_loc, d_model = x_rows.shape
        experts = logits.shape[1]
        num_local = experts // n
        cap = tok_loc * n * CAP_FACTOR // experts
        pair_cap = 2 * tok_loc * CAP_FACTOR // n
        ff = w_in.shape[2]
        tokens, rows_total, slots = n * tok_loc, num_local * cap, n * pair_cap
        nu = d_model // UNIT
        hbm = pl.BlockSpec(memory_space=pl.ANY)
        dma = pltpu.SemaphoreType.DMA
        vmem = pltpu.VMEM
        return pl.pallas_call(
            functools.partial(layer_kernel, n),
            out_shape=pltpu.VMEM((tok_loc, d_model), BF16),
            in_specs=[hbm] * 6,
            out_specs=pl.BlockSpec(memory_space=pltpu.VMEM),
            scratch_shapes=[
                vmem((nu, tokens, UNIT), BF16),
                vmem((rows_total, tokens), BF16),
                vmem((slots, rows_total), BF16),
                vmem((SEND_SLOTS, slots, UNIT), BF16),
                vmem((2, rows_total, UNIT), BF16),
                vmem((rows_total, ff), F32),
                vmem((W1_DEPTH, EXPERT_GROUP, UNIT, ff), BF16),
                vmem((W2_DEPTH, EXPERT_GROUP, ff, UNIT), BF16),
                vmem((rows_total, UNIT), BF16),
                vmem((rows_total, ff), BF16),
                vmem((tok_loc, shared_in.shape[1]), BF16),
                vmem(shared_in.shape, BF16),
                vmem(shared_out.shape, BF16),
                vmem((tok_loc, experts), F32),
                vmem((tok_loc, experts), F32),
                vmem((128, experts), F32),
                vmem((n, num_local, 128), F32),
                vmem((n, num_local, 128), F32),
                vmem((n, num_local, 128), F32),
                vmem((n, num_local, 128), F32),
                vmem((n, num_local, 128), F32),
                vmem((8, rows_total), F32),
                vmem((n, 8, pair_cap), F32),
                vmem((n, 8, pair_cap), F32),
                dma((nu,)), dma((3,)), dma((n,)), dma((n,)), dma((nu, KINDS)), dma((nu, KINDS)),
                dma((W1_DEPTH,)), dma((W2_DEPTH,)), dma((n,)), dma((n,)), dma((nu, n)), dma((nu, n)), pltpu.SemaphoreType.REGULAR,
            ],
            compiler_params=pltpu.CompilerParams(collective_id=0, has_side_effects=True, vmem_limit_bytes=VMEM_BYTES),
            name="moe_layer",
        )(x_rows, logits, w_in, shared_in, w_out, shared_out)

    row_spec = P(("dp", "ep"), None)
    expert_spec = P("ep", None, None)
    return jax.shard_map(local_layer, mesh=mesh, in_specs=(row_spec, row_spec, expert_spec, expert_spec, P(None, None), P(None, None)), out_specs=row_spec, check_vma=False)
```

```python
import functools

import jax
import jax.numpy as jnp
from jax import lax
from jax.experimental import pallas as pl
from jax.experimental.pallas import tpu as pltpu
from jax.sharding import PartitionSpec as P

CAP_FACTOR = 2
MESH = pl.DeviceIdType.MESH
F32 = jnp.float32
BF16 = jnp.bfloat16
VMEM_BYTES = 60 * 1024 * 1024
EXPERT_GROUP = 8
UNIT = 256
SEND_SLOTS = 3
W1_DEPTH = 5
W2_DEPTH = 4
KINDS = 9
COMBINE_ROWS = 256
GATHER_ROWS = 512


def dot(a, b):
    return jnp.dot(a, b, preferred_element_type=F32)


def gelu(v):
    return jax.nn.gelu(v)


def tile(i, size):
    return pl.ds(pl.multiple_of(i * size, size), size)


def layer_kernel(n, x_hbm, lg_hbm, w1_hbm, ws1_hbm, w2_hbm, ws2_hbm, out_ref,
                 xb, pick, sel, sendb, xg, hacc, w1buf, w2buf, z, h, hsb, ws2,
                 sc, gate_p, cand, cand_t, cand_r, m_sc, m_tok, m_gate, route, metas, metar,
                 x_sem, in_sem, c_ss, c_rs, ss, rs, w1_sem, w2_sem, m_ss, m_rs, a_ss, a_rs, free_sem):
    me = lax.axis_index("ep")
    core = lax.rem(me, 2)
    partner = me + 1 - 2 * core
    right, left = lax.rem(me + 2, n), lax.rem(me + n - 2, n)
    far = lax.rem(me + 4, n)
    tok_loc, d_model = x_hbm.shape
    num_local, _, ff = w1_hbm.shape
    nu = d_model // UNIT
    half = tok_loc // 2
    rows_total = hacc.shape[0]
    cap = rows_total // num_local
    slots = sel.shape[0]
    pair_cap = slots // n
    groups = num_local // EXPERT_GROUP
    steps = nu * groups

    def flip(d):
        return d + 1 - 2 * core

    def w1_copy(step):
        u, g, slot = step // groups, lax.rem(step, groups), lax.rem(step, W1_DEPTH)
        return pltpu.make_async_copy(w1_hbm.at[tile(g, EXPERT_GROUP), tile(u, UNIT), :], w1buf.at[slot], w1_sem.at[slot])

    def w2_copy(step):
        u, g, slot = step // groups, lax.rem(step, groups), lax.rem(step, W2_DEPTH)
        return pltpu.make_async_copy(w2_hbm.at[tile(g, EXPERT_GROUP), :, tile(u, UNIT)], w2buf.at[slot], w2_sem.at[slot])

    own = tile(me, tok_loc)
    x_copies = [pltpu.make_async_copy(x_hbm.at[:, pl.ds(u * UNIT, UNIT)], xb.at[u, own], x_sem.at[u]) for u in range(nu)]
    lg_copy = pltpu.make_async_copy(lg_hbm, sc, in_sem.at[0])
    ws2_copy = pltpu.make_async_copy(ws2_hbm, ws2, in_sem.at[2])
    for cp in x_copies + [lg_copy]:
        cp.start()
    barrier = pltpu.get_barrier_semaphore()
    for i in range(1, n):
        pl.semaphore_signal(barrier, inc=1, device_id={"ep": lax.rem(me + i, n)}, device_id_type=MESH)
    for cp in x_copies:
        cp.wait()
    pl.semaphore_wait(barrier, n - 1)

    def hop(u, kind, block, part, to):
        rows = tile(block, tok_loc) if part is None else tile(2 * block + part, half)
        ref = xb.at[u, rows]
        return pltpu.make_async_remote_copy(src_ref=ref, dst_ref=ref, send_sem=ss.at[u, kind], recv_sem=rs.at[u, kind], device_id={"ep": to}, device_id_type=MESH)

    def send_own(u):
        hop(u, 0, me, None, right).start()
        hop(u, 1, me, None, left).start()
        hop(u, 2, me, None, partner).start()

    def forward_near(u):
        hop(u, 0, left, None, partner).wait_recv()
        hop(u, 5, left, 0, right).start()
        hop(u, 3, left, None, partner).start()
        hop(u, 1, right, None, partner).wait_recv()
        hop(u, 6, right, 1, left).start()
        hop(u, 4, right, None, partner).start()

    def forward_far(u):
        hop(u, 5, far, 0, partner).wait_recv()
        hop(u, 7, far, 0, partner).start()
        hop(u, 6, far, 1, partner).wait_recv()
        hop(u, 8, far, 1, partner).start()

    def land_near(u):
        hop(u, 2, partner, None, partner).wait_recv()
        hop(u, 3, flip(left), None, partner).wait_recv()
        hop(u, 4, flip(right), None, partner).wait_recv()

    def land_far(u):
        hop(u, 7, flip(far), 0, partner).wait_recv()
        hop(u, 8, flip(far), 1, partner).wait_recv()

    send_own(0)
    send_own(1)
    for step in range(W1_DEPTH - 1):
        w1_copy(step).start()
    for step in range(W2_DEPTH - 1):
        w2_copy(step).start()

    lg_copy.wait()
    ws2_copy.start()
    raw = sc[...]
    ex = jnp.exp(raw - jnp.max(raw, axis=1, keepdims=True))
    gate_p[...] = ex / jnp.sum(ex, axis=1, keepdims=True)
    cand[...] = jnp.zeros_like(cand)
    tok_iota = lax.broadcasted_iota(jnp.int32, sc.shape, 0).astype(F32)

    def best_local(j, top):
        cur = sc[...]
        hit = cur == top
        cand[pl.ds(j, 1), :] = top
        cand[pl.ds(cap + j, 1), :] = jnp.sum(jnp.where(hit, tok_iota, 0.0), axis=0, keepdims=True)
        cand[pl.ds(2 * cap + j, 1), :] = jnp.sum(jnp.where(hit, gate_p[...], 0.0), axis=0, keepdims=True)
        cur = jnp.where(hit, -jnp.inf, cur)
        sc[...] = cur
        return jnp.max(cur, axis=0, keepdims=True)

    lax.fori_loop(0, cap, best_local, jnp.max(raw, axis=0, keepdims=True))

    flat_t = cand[...].T
    for d in range(n):
        cand_t[d] = flat_t[d * num_local:(d + 1) * num_local]
    cand_r[me] = cand_t[me]
    cand_copies = []
    for i in range(1, n):
        dst = lax.rem(me + i, n)
        cp = pltpu.make_async_remote_copy(src_ref=cand_t.at[dst], dst_ref=cand_r.at[me], send_sem=c_ss.at[i], recv_sem=c_rs.at[i], device_id={"ep": dst}, device_id_type=MESH)
        cp.start()
        cand_copies.append(cp)

    forward_near(0)
    send_own(2)

    forward_near(1)
    send_own(3)

    for cp in cand_copies:
        cp.wait()
    lane = lax.broadcasted_iota(jnp.int32, (num_local, 128), 1)
    for s in range(n):
        block = cand_r[s]
        m_sc[s] = jnp.where(lane < cap, block, -jnp.inf)
        m_tok[s] = pltpu.roll(block, 128 - cap, 1) + float(s) * tok_loc
        m_gate[s] = pltpu.roll(block, 128 - 2 * cap, 1)

    per_row = 128 // cap
    home = lax.rem(lax.broadcasted_iota(jnp.int32, (num_local, 128), 0), per_row) * cap

    def extract(j, carry):
        tok_tab, gate_tab = carry
        cur = m_sc[...]
        top = jnp.max(jnp.max(cur, axis=0), axis=1, keepdims=True)
        hit = cur == top[None]
        tok = jnp.sum(jnp.sum(jnp.where(hit, m_tok[...], 0.0), axis=0), axis=1, keepdims=True)
        gate = jnp.sum(jnp.sum(jnp.where(hit, m_gate[...], 0.0), axis=0), axis=1, keepdims=True)
        m_sc[...] = jnp.where(hit, -jnp.inf, cur)
        here = lane == home + j
        return jnp.where(here, tok, tok_tab), jnp.where(here, gate, gate_tab)

    zero = jnp.zeros((num_local, 128), F32)
    tok_tab, gate_tab = lax.fori_loop(0, cap, extract, (zero, zero))
    nrow = num_local // per_row
    tok_rows = [jnp.sum(tok_tab[g * per_row:(g + 1) * per_row], axis=0, keepdims=True) for g in range(nrow)]
    gate_rows = [jnp.sum(gate_tab[g * per_row:(g + 1) * per_row], axis=0, keepdims=True) for g in range(nrow)]
    tok_flat = jnp.concatenate(tok_rows, axis=1)
    gate_flat = jnp.concatenate(gate_rows, axis=1)

    tok_cols = jnp.concatenate(tok_rows, axis=0).T
    for g in range(nrow):
        col = tok_cols[:, g:g + 1]

        @pl.loop(0, n)
        def _(s):
            ids = lax.broadcasted_iota(jnp.int32, (128, tok_loc), 1).astype(F32) + (s * tok_loc).astype(F32)
            pick[pl.ds(g * 128, 128), tile(s, tok_loc)] = jnp.where(ids == col, 1.0, 0.0).astype(BF16)

    route[6:7, :] = tok_flat
    route[7:8, :] = gate_flat

    def meta_copy(i):
        dst = lax.rem(me + i, n)
        return pltpu.make_async_remote_copy(src_ref=metas.at[dst], dst_ref=metar.at[me], send_sem=m_ss.at[i], recv_sem=m_rs.at[i], device_id={"ep": dst}, device_id_type=MESH)

    def announce():
        tok_flat, gate_flat = route[6:7, :], route[7:8, :]
        source = jnp.floor(tok_flat * (1.0 / tok_loc))
        loc = tok_flat - source * tok_loc
        of_src = jnp.where(lax.broadcasted_iota(jnp.int32, (n, rows_total), 0).astype(F32) == source, 1.0, 0.0)
        sq = (rows_total, rows_total)
        before = jnp.where(lax.broadcasted_iota(jnp.int32, sq, 0) < lax.broadcasted_iota(jnp.int32, sq, 1), 1.0, 0.0).astype(BF16)
        slot = jnp.sum(of_src * dot(of_src.astype(BF16), before), axis=0, keepdims=True)
        hi = jnp.floor(loc * (1.0 / 16))
        g_hi = gate_flat.astype(BF16).astype(F32)
        g_mid = (gate_flat - g_hi).astype(BF16).astype(F32)
        route[0:1, :] = hi
        route[1:2, :] = loc - 16 * hi
        route[2:3, :] = jnp.ones_like(hi)
        route[3:4, :] = g_hi
        route[4:5, :] = g_mid
        route[5:6, :] = gate_flat - g_hi - g_mid
        route[6:7, :] = source * pair_cap + slot
        route[7:8, :] = jnp.zeros_like(hi)

        for g in range(rows_total // 128):
            key = route[6:7, g * 128:(g + 1) * 128]

            @pl.loop(0, slots // 256)
            def _(t):
                ids = lax.broadcasted_iota(jnp.int32, (256, 128), 0).astype(F32) + (t * 256).astype(F32)
                sel[tile(t, 256), pl.ds(g * 128, 128)] = jnp.where(ids == key, 1.0, 0.0).astype(BF16)

        vals = route[...].astype(BF16)

        @pl.loop(0, n)
        def _(d):
            metas[d] = lax.dot_general(vals, sel[tile(d, pair_cap), :], (((1,), (1,)), ((), ())), preferred_element_type=F32)

        metar[me] = metas[me]
        for i in range(1, n):
            meta_copy(i).start()

    hacc[...] = jnp.zeros_like(hacc)
    chip = 2 * tok_loc
    near_chips = [lax.rem(me // 2 + k, n // 2) for k in (0, 1, n // 2 - 1)]
    far_chip = far // 2

    def gather_near(u):
        land_near(u)

        @pl.loop(0, rows_total // GATHER_ROWS)
        def _(t):
            rows = tile(t, GATHER_ROWS)
            acc = dot(pick[rows, tile(near_chips[0], chip)], xb[u, tile(near_chips[0], chip), :])
            for q in near_chips[1:]:
                acc += dot(pick[rows, tile(q, chip)], xb[u, tile(q, chip), :])
            xg[lax.rem(u, 2), rows, :] = acc.astype(BF16)

    def gather_far(u):
        land_far(u)

        @pl.loop(0, rows_total // GATHER_ROWS)
        def _(t):
            rows = tile(t, GATHER_ROWS)
            acc = dot(pick[rows, tile(far_chip, chip)], xb[u, tile(far_chip, chip), :])
            xg[lax.rem(u, 2), rows, :] = (xg[lax.rem(u, 2), rows, :].astype(F32) + acc).astype(BF16)

    def gather(u):
        land_near(u)
        land_far(u)

        @pl.loop(0, rows_total // GATHER_ROWS)
        def _(t):
            rows = tile(t, GATHER_ROWS)
            xg[lax.rem(u, 2), rows, :] = dot(pick[rows, :], xb[u]).astype(BF16)

    def next_w1(step):
        @pl.when(step + W1_DEPTH - 1 < steps)
        def _():
            w1_copy(step + W1_DEPTH - 1).start()

        w1_copy(step).wait()
        return lax.rem(step, W1_DEPTH)

    def next_w2(step):
        @pl.when(step + W2_DEPTH - 1 < steps)
        def _():
            w2_copy(step + W2_DEPTH - 1).start()

        w2_copy(step).wait()
        return lax.rem(step, W2_DEPTH)

    def first_product(u, lo, hi_):
        @pl.loop(lo, hi_)
        def _(g):
            buf = next_w1(u * groups + g)
            for i in range(EXPERT_GROUP):
                rows = tile(g * EXPERT_GROUP + i, cap)
                hacc[rows, :] += dot(xg[lax.rem(u, 2), rows, :], w1buf[buf, i])

    def drain(u):
        hop(u, 0, me, None, right).wait_send()
        hop(u, 1, me, None, left).wait_send()
        hop(u, 2, me, None, partner).wait_send()
        hop(u, 3, left, None, partner).wait_send()
        hop(u, 4, right, None, partner).wait_send()
        hop(u, 5, left, 0, right).wait_send()
        hop(u, 6, right, 1, left).wait_send()
        hop(u, 7, far, 0, partner).wait_send()
        hop(u, 8, far, 1, partner).wait_send()

    forward_near(2)
    send_own(4)
    forward_far(0)
    gather(0)
    first_product(0, 0, groups)
    forward_far(1)
    gather(1)

    @pl.loop(3, nu - 1)
    def _(u):
        forward_near(u)

        @pl.when(u + 2 < nu)
        def _():
            send_own(u + 2)

        first_product(u - 2, 0, groups)
        drain(u - 3)
        forward_far(u - 1)
        gather(u - 1)

        @pl.when(u == 4)
        def _():
            announce()

    first_product(nu - 3, 0, groups)
    forward_near(nu - 1)
    gather_near(nu - 2)
    drain(nu - 4)
    drain(nu - 3)
    forward_far(nu - 2)
    gather_near(nu - 1)
    gather_far(nu - 2)
    forward_far(nu - 1)
    first_product(nu - 2, 0, groups)
    drain(nu - 2)
    gather_far(nu - 1)

    drain(nu - 1)
    for i in range(1, n):
        pl.semaphore_signal(free_sem, inc=1, device_id={"ep": lax.rem(me + i, n)}, device_id_type=MESH)

    @pl.loop(0, groups)
    def _(g):
        buf1, buf2 = next_w1((nu - 1) * groups + g), next_w2(g)
        for i in range(EXPERT_GROUP):
            rows = tile(g * EXPERT_GROUP + i, cap)
            act = gelu(hacc[rows, :] + dot(xg[(nu - 1) % 2, rows, :], w1buf[buf1, i])).astype(BF16)
            h[rows, :] = act
            z[rows, :] = dot(act, w2buf[buf2, i]).astype(BF16)

    ws1_copies = [pltpu.make_async_copy(ws1_hbm.at[pl.ds(u * UNIT, UNIT), :], w1buf.at[0, u], x_sem.at[u]) for u in range(nu)]
    for cp in ws1_copies:
        cp.start()
    pl.semaphore_wait(free_sem, n - 1)

    def landing(d):
        return (n // 2) * tok_loc * (1 - d // (n // 2))

    def back(u, i):
        dst = lax.rem(me + i, n)
        return pltpu.make_async_remote_copy(src_ref=sendb.at[lax.rem(u, SEND_SLOTS), tile(dst, pair_cap)], dst_ref=xb.at[u, pl.ds(pl.multiple_of(landing(dst) + me * pair_cap, pair_cap), pair_cap)], send_sem=a_ss.at[u, i], recv_sem=a_rs.at[u, i], device_id={"ep": dst}, device_id_type=MESH)

    def arrived(u, i):
        src = lax.rem(me + n - i, n)
        ref = xb.at[u, pl.ds(pl.multiple_of(landing(me) + src * pair_cap, pair_cap), pair_cap)]
        pltpu.make_async_remote_copy(src_ref=ref, dst_ref=ref, send_sem=a_ss.at[u, i], recv_sem=a_rs.at[u, i], device_id={"ep": partner}, device_id_type=MESH).wait_recv()

    def second_product(u):
        @pl.loop(0, groups)
        def _(g):
            buf = next_w2(u * groups + g)
            for i in range(EXPERT_GROUP):
                rows = tile(g * EXPERT_GROUP + i, cap)
                z[rows, :] = dot(h[rows, :], w2buf[buf, i]).astype(BF16)

    def send_back(u):
        @pl.when(u >= SEND_SLOTS)
        def _():
            for i in range(1, n):
                back(u - SEND_SLOTS, i).wait_send()

        pair = 2 * pair_cap
        chip_me = me // 2

        for k in (1, n // 2 - 1, 2):
            q = lax.rem(chip_me + k, n // 2)
            sendb[lax.rem(u, SEND_SLOTS), tile(q, pair), :] = dot(sel[tile(q, pair), :], z[...]).astype(BF16)
            back(u, lax.rem(2 * q - me + n, n)).start()
            back(u, lax.rem(2 * q + 1 - me + n, n)).start()

        sendb[lax.rem(u, SEND_SLOTS), tile(partner, pair_cap), :] = dot(sel[tile(partner, pair_cap), :], z[...]).astype(BF16)
        back(u, lax.rem(partner - me + n, n)).start()
        xb[u, pl.ds(pl.multiple_of(landing(me) + me * pair_cap, pair_cap), pair_cap), :] = dot(sel[tile(me, pair_cap), :], z[...]).astype(BF16)

    def weights_at(k):
        return (tok_loc if k == 1 else 0), (slots if k == 2 else 0)

    def build_weights():
        for i in range(1, n):
            meta_copy(i).wait()

        @pl.loop(0, n)
        def _(o):
            tok = 16.0 * metar[o, 0:1, :] + metar[o, 1:2, :] + metar[o, 2:3, :] - 1.0
            hit = lax.broadcasted_iota(jnp.int32, (tok_loc, pair_cap), 0).astype(F32) == tok
            for k in range(3):
                r0, c0 = weights_at(k)
                pick[pl.ds(r0, tok_loc), pl.ds(pl.multiple_of(c0 + o * pair_cap, pair_cap), pair_cap)] = jnp.where(hit, metar[o, 3 + k:4 + k, :], 0.0).astype(BF16)

    def finish(u, last=False):
        pair = 2 * pair_cap

        def shared(rows):
            return dot(hsb[rows, :], ws2[:, tile(u, UNIT)]).astype(BF16).astype(F32)

        def weighted(t, acc, q):
            for part in range(3):
                r0, c0 = weights_at(part)
                lhs_rows = pl.ds(pl.multiple_of(r0 + t * COMBINE_ROWS, COMBINE_ROWS), COMBINE_ROWS)
                if q is None:
                    acc += dot(pick[lhs_rows, c0:c0 + slots], xb[u, pl.ds(pl.multiple_of(landing(me), slots), slots), :])
                else:
                    acc += dot(pick[lhs_rows, pl.ds(pl.multiple_of(c0 + q * pair, pair), pair)], xb[u, pl.ds(pl.multiple_of(landing(me) + q * pair, pair), pair), :])
            return acc

        def write(t, acc):
            x_own = xb[u, pl.ds(pl.multiple_of(me * tok_loc + t * COMBINE_ROWS, COMBINE_ROWS), COMBINE_ROWS), :].astype(F32)
            out_ref[tile(t, COMBINE_ROWS), tile(u, UNIT)] = (x_own + acc).astype(BF16)

        def chip_arrived(q):
            arrived(u, lax.rem(me + n - 2 * q, n))
            arrived(u, lax.rem(me + n - 2 * q - 1 + n, n))

        arrived(u, lax.rem(me + n - partner, n))
        chip_arrived(near_chips[1])
        chip_arrived(near_chips[2])
        if last:
            @pl.loop(0, tok_loc // COMBINE_ROWS)
            def _(t):
                acc = shared(tile(t, COMBINE_ROWS))
                for q in near_chips:
                    acc = weighted(t, acc, q)
                hacc[tile(t, COMBINE_ROWS), 0:UNIT] = acc

            chip_arrived(far_chip)

            @pl.loop(0, tok_loc // COMBINE_ROWS)
            def _(t):
                write(t, weighted(t, hacc[tile(t, COMBINE_ROWS), 0:UNIT], far_chip))
        else:
            chip_arrived(far_chip)

            @pl.loop(0, tok_loc // COMBINE_ROWS)
            def _(t):
                write(t, weighted(t, shared(tile(t, COMBINE_ROWS)), None))


    send_back(0)
    build_weights()
    for cp in ws1_copies:
        cp.wait()
    ws2_copy.wait()

    @pl.loop(0, tok_loc // 128)
    def _(t):
        rows = pl.ds(pl.multiple_of(me * tok_loc + t * 128, 128), 128)
        acc = dot(xb[0, rows, :], w1buf[0, 0])
        for u in range(1, nu):
            acc += dot(xb[u, rows, :], w1buf[0, u])
        hsb[tile(t, 128), :] = gelu(acc).astype(BF16)


    @pl.loop(1, nu)
    def _(u):
        second_product(u)
        send_back(u)
        finish(u - 1)

    finish(nu - 1, True)

    @pl.loop(nu - SEND_SLOTS, nu)
    def _(u):
        for i in range(1, n):
            back(u, i).wait_send()


def solution(mesh):
    n = mesh.shape["ep"]

    def local_layer(x_rows, logits, w_in, w_out, shared_in, shared_out):
        tok_loc, d_model = x_rows.shape
        experts = logits.shape[1]
        num_local = experts // n
        cap = tok_loc * n * CAP_FACTOR // experts
        pair_cap = 2 * tok_loc * CAP_FACTOR // n
        ff = w_in.shape[2]
        tokens, rows_total, slots = n * tok_loc, num_local * cap, n * pair_cap
        nu = d_model // UNIT
        hbm = pl.BlockSpec(memory_space=pl.ANY)
        dma = pltpu.SemaphoreType.DMA
        vmem = pltpu.VMEM
        return pl.pallas_call(
            functools.partial(layer_kernel, n),
            out_shape=pltpu.VMEM((tok_loc, d_model), BF16),
            in_specs=[hbm] * 6,
            out_specs=pl.BlockSpec(memory_space=pltpu.VMEM),
            scratch_shapes=[
                vmem((nu, tokens, UNIT), BF16),
                vmem((rows_total, tokens), BF16),
                vmem((slots, rows_total), BF16),
                vmem((SEND_SLOTS, slots, UNIT), BF16),
                vmem((2, rows_total, UNIT), BF16),
                vmem((rows_total, ff), F32),
                vmem((W1_DEPTH, EXPERT_GROUP, UNIT, ff), BF16),
                vmem((W2_DEPTH, EXPERT_GROUP, ff, UNIT), BF16),
                vmem((rows_total, UNIT), BF16),
                vmem((rows_total, ff), BF16),
                vmem((tok_loc, shared_in.shape[1]), BF16),
                vmem(shared_out.shape, BF16),
                vmem((tok_loc, experts), F32),
                vmem((tok_loc, experts), F32),
                vmem((128, experts), F32),
                vmem((n, num_local, 128), F32),
                vmem((n, num_local, 128), F32),
                vmem((n, num_local, 128), F32),
                vmem((n, num_local, 128), F32),
                vmem((n, num_local, 128), F32),
                vmem((8, rows_total), F32),
                vmem((n, 8, pair_cap), F32),
                vmem((n, 8, pair_cap), F32),
                dma((nu,)), dma((3,)), dma((n,)), dma((n,)), dma((nu, KINDS)), dma((nu, KINDS)),
                dma((W1_DEPTH,)), dma((W2_DEPTH,)), dma((n,)), dma((n,)), dma((nu, n)), dma((nu, n)), pltpu.SemaphoreType.REGULAR,
            ],
            compiler_params=pltpu.CompilerParams(collective_id=0, has_side_effects=True, vmem_limit_bytes=VMEM_BYTES),
            name="moe_layer",
        )(x_rows, logits, w_in, shared_in, w_out, shared_out)

    row_spec = P(("dp", "ep"), None)
    expert_spec = P("ep", None, None)
    return jax.shard_map(local_layer, mesh=mesh, in_specs=(row_spec, row_spec, expert_spec, expert_spec, P(None, None), P(None, None)), out_specs=row_spec, check_vma=False)
```

```python
import functools

import jax
import jax.numpy as jnp
from jax import lax
from jax.experimental import pallas as pl
from jax.experimental.pallas import tpu as pltpu
from jax.sharding import PartitionSpec as P

CAP_FACTOR = 2
MESH = pl.DeviceIdType.MESH
F32 = jnp.float32
BF16 = jnp.bfloat16
VMEM_BYTES = 60 * 1024 * 1024
EXPERT_GROUP = 8
UNIT = 256
SEND_SLOTS = 3
W1_DEPTH = 5
W2_DEPTH = 4
KINDS = 9
COMBINE_ROWS = 256
GATHER_ROWS = 512


def dot(a, b):
    return jnp.dot(a, b, preferred_element_type=F32)


def gelu(v):
    return jax.nn.gelu(v)


def tile(i, size):
    return pl.ds(pl.multiple_of(i * size, size), size)


def layer_kernel(n, x_hbm, lg_hbm, w1_hbm, ws1_hbm, w2_hbm, ws2_hbm, out_ref,
                 xb, pick, sel, sendb, xg, hacc, w1buf, w2buf, z, h, hsb, ws2,
                 sc, gate_p, cand, cand_t, cand_r, m_sc, m_tok, m_gate, route, metas, metar,
                 x_sem, in_sem, c_ss, c_rs, ss, rs, w1_sem, w2_sem, m_ss, m_rs, a_ss, a_rs, free_sem):
    me = lax.axis_index("ep")
    core = lax.rem(me, 2)
    partner = me + 1 - 2 * core
    right, left = lax.rem(me + 2, n), lax.rem(me + n - 2, n)
    far = lax.rem(me + 4, n)
    tok_loc, d_model = x_hbm.shape
    num_local, _, ff = w1_hbm.shape
    nu = d_model // UNIT
    half = tok_loc // 2
    rows_total = hacc.shape[0]
    cap = rows_total // num_local
    slots = sel.shape[0]
    pair_cap = slots // n
    groups = num_local // EXPERT_GROUP
    steps = nu * groups

    def flip(d):
        return d + 1 - 2 * core

    def w1_copy(step):
        u, g, slot = step // groups, lax.rem(step, groups), lax.rem(step, W1_DEPTH)
        return pltpu.make_async_copy(w1_hbm.at[tile(g, EXPERT_GROUP), tile(u, UNIT), :], w1buf.at[slot], w1_sem.at[slot])

    def w2_copy(step):
        u, g, slot = step // groups, lax.rem(step, groups), lax.rem(step, W2_DEPTH)
        return pltpu.make_async_copy(w2_hbm.at[tile(g, EXPERT_GROUP), :, tile(u, UNIT)], w2buf.at[slot], w2_sem.at[slot])

    own = tile(me, tok_loc)
    x_copies = [pltpu.make_async_copy(x_hbm.at[:, pl.ds(u * UNIT, UNIT)], xb.at[u, own], x_sem.at[u]) for u in range(nu)]
    lg_copy = pltpu.make_async_copy(lg_hbm, sc, in_sem.at[0])
    ws2_copy = pltpu.make_async_copy(ws2_hbm, ws2, in_sem.at[2])
    barrier = pltpu.get_barrier_semaphore()
    for i in range(1, n):
        pl.semaphore_signal(barrier, inc=1, device_id={"ep": lax.rem(me + i, n)}, device_id_type=MESH)
    for cp in x_copies + [lg_copy]:
        cp.start()
    pl.semaphore_wait(barrier, n - 1)

    def hop(u, kind, block, part, to):
        rows = tile(block, tok_loc) if part is None else tile(2 * block + part, half)
        ref = xb.at[u, rows]
        return pltpu.make_async_remote_copy(src_ref=ref, dst_ref=ref, send_sem=ss.at[u, kind], recv_sem=rs.at[u, kind], device_id={"ep": to}, device_id_type=MESH)

    def send_own(u):
        hop(u, 0, me, None, right).start()
        hop(u, 1, me, None, left).start()
        hop(u, 2, me, None, partner).start()

    def forward_near(u):
        hop(u, 0, left, None, partner).wait_recv()
        hop(u, 5, left, 0, right).start()
        hop(u, 3, left, None, partner).start()
        hop(u, 1, right, None, partner).wait_recv()
        hop(u, 6, right, 1, left).start()
        hop(u, 4, right, None, partner).start()

    def forward_far(u):
        hop(u, 5, far, 0, partner).wait_recv()
        hop(u, 7, far, 0, partner).start()
        hop(u, 6, far, 1, partner).wait_recv()
        hop(u, 8, far, 1, partner).start()

    def land_near(u):
        hop(u, 2, partner, None, partner).wait_recv()
        hop(u, 3, flip(left), None, partner).wait_recv()
        hop(u, 4, flip(right), None, partner).wait_recv()

    def land_far(u):
        hop(u, 7, flip(far), 0, partner).wait_recv()
        hop(u, 8, flip(far), 1, partner).wait_recv()

    x_copies[0].wait()
    send_own(0)
    x_copies[1].wait()
    send_own(1)
    for cp in x_copies[2:]:
        cp.wait()
    for step in range(W1_DEPTH - 1):
        w1_copy(step).start()
    for step in range(W2_DEPTH - 1):
        w2_copy(step).start()

    lg_copy.wait()
    ws2_copy.start()
    raw = sc[...]
    ex = jnp.exp(raw - jnp.max(raw, axis=1, keepdims=True))
    gate_p[...] = ex / jnp.sum(ex, axis=1, keepdims=True)
    cand[...] = jnp.zeros_like(cand)
    tok_iota = lax.broadcasted_iota(jnp.int32, sc.shape, 0).astype(F32)

    def best_local(j, top):
        cur = sc[...]
        hit = cur == top
        cand[pl.ds(j, 1), :] = top
        cand[pl.ds(cap + j, 1), :] = jnp.sum(jnp.where(hit, tok_iota, 0.0), axis=0, keepdims=True)
        cand[pl.ds(2 * cap + j, 1), :] = jnp.sum(jnp.where(hit, gate_p[...], 0.0), axis=0, keepdims=True)
        cur = jnp.where(hit, -jnp.inf, cur)
        sc[...] = cur
        return jnp.max(cur, axis=0, keepdims=True)

    lax.fori_loop(0, cap, best_local, jnp.max(raw, axis=0, keepdims=True))

    flat_t = cand[...].T
    for d in range(n):
        cand_t[d] = flat_t[d * num_local:(d + 1) * num_local]
    cand_r[me] = cand_t[me]
    cand_copies = []
    for i in range(1, n):
        dst = lax.rem(me + i, n)
        cp = pltpu.make_async_remote_copy(src_ref=cand_t.at[dst], dst_ref=cand_r.at[me], send_sem=c_ss.at[i], recv_sem=c_rs.at[i], device_id={"ep": dst}, device_id_type=MESH)
        cp.start()
        cand_copies.append(cp)

    forward_near(0)
    send_own(2)

    forward_near(1)
    send_own(3)

    for cp in cand_copies:
        cp.wait()
    lane = lax.broadcasted_iota(jnp.int32, (num_local, 128), 1)
    for s in range(n):
        block = cand_r[s]
        m_sc[s] = jnp.where(lane < cap, block, -jnp.inf)
        m_tok[s] = pltpu.roll(block, 128 - cap, 1) + float(s) * tok_loc
        m_gate[s] = pltpu.roll(block, 128 - 2 * cap, 1)

    per_row = 128 // cap
    home = lax.rem(lax.broadcasted_iota(jnp.int32, (num_local, 128), 0), per_row) * cap

    def extract(j, carry):
        tok_tab, gate_tab = carry
        cur = m_sc[...]
        top = jnp.max(jnp.max(cur, axis=0), axis=1, keepdims=True)
        hit = cur == top[None]
        tok = jnp.sum(jnp.sum(jnp.where(hit, m_tok[...], 0.0), axis=0), axis=1, keepdims=True)
        gate = jnp.sum(jnp.sum(jnp.where(hit, m_gate[...], 0.0), axis=0), axis=1, keepdims=True)
        m_sc[...] = jnp.where(hit, -jnp.inf, cur)
        here = lane == home + j
        return jnp.where(here, tok, tok_tab), jnp.where(here, gate, gate_tab)

    zero = jnp.zeros((num_local, 128), F32)
    tok_tab, gate_tab = lax.fori_loop(0, cap, extract, (zero, zero))
    nrow = num_local // per_row
    tok_rows = [jnp.sum(tok_tab[g * per_row:(g + 1) * per_row], axis=0, keepdims=True) for g in range(nrow)]
    gate_rows = [jnp.sum(gate_tab[g * per_row:(g + 1) * per_row], axis=0, keepdims=True) for g in range(nrow)]
    tok_flat = jnp.concatenate(tok_rows, axis=1)
    gate_flat = jnp.concatenate(gate_rows, axis=1)

    tok_cols = jnp.concatenate(tok_rows, axis=0).T
    for g in range(nrow):
        col = tok_cols[:, g:g + 1]

        @pl.loop(0, n)
        def _(s):
            ids = lax.broadcasted_iota(jnp.int32, (128, tok_loc), 1).astype(F32) + (s * tok_loc).astype(F32)
            pick[pl.ds(g * 128, 128), tile(s, tok_loc)] = jnp.where(ids == col, 1.0, 0.0).astype(BF16)

    route[6:7, :] = tok_flat
    route[7:8, :] = gate_flat

    def meta_copy(i):
        dst = lax.rem(me + i, n)
        return pltpu.make_async_remote_copy(src_ref=metas.at[dst], dst_ref=metar.at[me], send_sem=m_ss.at[i], recv_sem=m_rs.at[i], device_id={"ep": dst}, device_id_type=MESH)

    def announce():
        tok_flat, gate_flat = route[6:7, :], route[7:8, :]
        source = jnp.floor(tok_flat * (1.0 / tok_loc))
        loc = tok_flat - source * tok_loc
        of_src = jnp.where(lax.broadcasted_iota(jnp.int32, (n, rows_total), 0).astype(F32) == source, 1.0, 0.0)
        sq = (rows_total, rows_total)
        before = jnp.where(lax.broadcasted_iota(jnp.int32, sq, 0) < lax.broadcasted_iota(jnp.int32, sq, 1), 1.0, 0.0).astype(BF16)
        slot = jnp.sum(of_src * dot(of_src.astype(BF16), before), axis=0, keepdims=True)
        hi = jnp.floor(loc * (1.0 / 16))
        g_hi = gate_flat.astype(BF16).astype(F32)
        g_mid = (gate_flat - g_hi).astype(BF16).astype(F32)
        route[0:1, :] = hi
        route[1:2, :] = loc - 16 * hi
        route[2:3, :] = jnp.ones_like(hi)
        route[3:4, :] = g_hi
        route[4:5, :] = g_mid
        route[5:6, :] = gate_flat - g_hi - g_mid
        route[6:7, :] = source * pair_cap + slot
        route[7:8, :] = jnp.zeros_like(hi)

        for g in range(rows_total // 128):
            key = route[6:7, g * 128:(g + 1) * 128]

            @pl.loop(0, slots // 256)
            def _(t):
                ids = lax.broadcasted_iota(jnp.int32, (256, 128), 0).astype(F32) + (t * 256).astype(F32)
                sel[tile(t, 256), pl.ds(g * 128, 128)] = jnp.where(ids == key, 1.0, 0.0).astype(BF16)

        vals = route[...].astype(BF16)

        @pl.loop(0, n)
        def _(d):
            metas[d] = lax.dot_general(vals, sel[tile(d, pair_cap), :], (((1,), (1,)), ((), ())), preferred_element_type=F32)

        metar[me] = metas[me]
        for i in range(1, n):
            meta_copy(i).start()

    hacc[...] = jnp.zeros_like(hacc)
    chip = 2 * tok_loc
    near_chips = [lax.rem(me // 2 + k, n // 2) for k in (0, 1, n // 2 - 1)]
    far_chip = far // 2

    def gather_near(u):
        land_near(u)

        @pl.loop(0, rows_total // GATHER_ROWS)
        def _(t):
            rows = tile(t, GATHER_ROWS)
            acc = dot(pick[rows, tile(near_chips[0], chip)], xb[u, tile(near_chips[0], chip), :])
            for q in near_chips[1:]:
                acc += dot(pick[rows, tile(q, chip)], xb[u, tile(q, chip), :])
            xg[lax.rem(u, 2), rows, :] = acc.astype(BF16)

    def gather_far(u):
        land_far(u)

        @pl.loop(0, rows_total // GATHER_ROWS)
        def _(t):
            rows = tile(t, GATHER_ROWS)
            acc = dot(pick[rows, tile(far_chip, chip)], xb[u, tile(far_chip, chip), :])
            xg[lax.rem(u, 2), rows, :] = (xg[lax.rem(u, 2), rows, :].astype(F32) + acc).astype(BF16)

    def gather(u):
        land_near(u)
        land_far(u)

        @pl.loop(0, rows_total // GATHER_ROWS)
        def _(t):
            rows = tile(t, GATHER_ROWS)
            xg[lax.rem(u, 2), rows, :] = dot(pick[rows, :], xb[u]).astype(BF16)

    def next_w1(step):
        @pl.when(step + W1_DEPTH - 1 < steps)
        def _():
            w1_copy(step + W1_DEPTH - 1).start()

        w1_copy(step).wait()
        return lax.rem(step, W1_DEPTH)

    def next_w2(step):
        @pl.when(step + W2_DEPTH - 1 < steps)
        def _():
            w2_copy(step + W2_DEPTH - 1).start()

        w2_copy(step).wait()
        return lax.rem(step, W2_DEPTH)

    def first_product(u, lo, hi_):
        @pl.loop(lo, hi_)
        def _(g):
            buf = next_w1(u * groups + g)
            for i in range(EXPERT_GROUP):
                rows = tile(g * EXPERT_GROUP + i, cap)
                hacc[rows, :] += dot(xg[lax.rem(u, 2), rows, :], w1buf[buf, i])

    def drain(u):
        hop(u, 0, me, None, right).wait_send()
        hop(u, 1, me, None, left).wait_send()
        hop(u, 2, me, None, partner).wait_send()
        hop(u, 3, left, None, partner).wait_send()
        hop(u, 4, right, None, partner).wait_send()
        hop(u, 5, left, 0, right).wait_send()
        hop(u, 6, right, 1, left).wait_send()
        hop(u, 7, far, 0, partner).wait_send()
        hop(u, 8, far, 1, partner).wait_send()

    forward_near(2)
    send_own(4)
    forward_far(0)
    gather(0)
    first_product(0, 0, groups)
    forward_far(1)
    gather(1)

    @pl.loop(3, nu - 1)
    def _(u):
        forward_near(u)

        @pl.when(u + 2 < nu)
        def _():
            send_own(u + 2)

        first_product(u - 2, 0, groups)
        drain(u - 3)
        forward_far(u - 1)
        gather(u - 1)

        @pl.when(u == 4)
        def _():
            announce()

    first_product(nu - 3, 0, groups)
    forward_near(nu - 1)
    gather_near(nu - 2)
    drain(nu - 4)
    drain(nu - 3)
    forward_far(nu - 2)
    gather_near(nu - 1)
    gather_far(nu - 2)
    forward_far(nu - 1)
    first_product(nu - 2, 0, groups)
    drain(nu - 2)
    gather_far(nu - 1)

    drain(nu - 1)
    for i in range(1, n):
        pl.semaphore_signal(free_sem, inc=1, device_id={"ep": lax.rem(me + i, n)}, device_id_type=MESH)

    @pl.loop(0, groups)
    def _(g):
        buf1, buf2 = next_w1((nu - 1) * groups + g), next_w2(g)
        for i in range(EXPERT_GROUP):
            rows = tile(g * EXPERT_GROUP + i, cap)
            act = gelu(hacc[rows, :] + dot(xg[(nu - 1) % 2, rows, :], w1buf[buf1, i])).astype(BF16)
            h[rows, :] = act
            z[rows, :] = dot(act, w2buf[buf2, i]).astype(BF16)

    ws1_copies = [pltpu.make_async_copy(ws1_hbm.at[pl.ds(u * UNIT, UNIT), :], w1buf.at[0, u], x_sem.at[u]) for u in range(nu)]
    for cp in ws1_copies:
        cp.start()
    pl.semaphore_wait(free_sem, n - 1)

    def landing(d):
        return (n // 2) * tok_loc * (1 - d // (n // 2))

    def back(u, i):
        dst = lax.rem(me + i, n)
        return pltpu.make_async_remote_copy(src_ref=sendb.at[lax.rem(u, SEND_SLOTS), tile(dst, pair_cap)], dst_ref=xb.at[u, pl.ds(pl.multiple_of(landing(dst) + me * pair_cap, pair_cap), pair_cap)], send_sem=a_ss.at[u, i], recv_sem=a_rs.at[u, i], device_id={"ep": dst}, device_id_type=MESH)

    def arrived(u, i):
        src = lax.rem(me + n - i, n)
        ref = xb.at[u, pl.ds(pl.multiple_of(landing(me) + src * pair_cap, pair_cap), pair_cap)]
        pltpu.make_async_remote_copy(src_ref=ref, dst_ref=ref, send_sem=a_ss.at[u, i], recv_sem=a_rs.at[u, i], device_id={"ep": partner}, device_id_type=MESH).wait_recv()

    def second_product(u):
        @pl.loop(0, groups)
        def _(g):
            buf = next_w2(u * groups + g)
            for i in range(EXPERT_GROUP):
                rows = tile(g * EXPERT_GROUP + i, cap)
                z[rows, :] = dot(h[rows, :], w2buf[buf, i]).astype(BF16)

    def send_back(u):
        @pl.when(u >= SEND_SLOTS)
        def _():
            for i in range(1, n):
                back(u - SEND_SLOTS, i).wait_send()

        pair = 2 * pair_cap
        chip_me = me // 2

        for k in (1, n // 2 - 1, 2):
            q = lax.rem(chip_me + k, n // 2)
            sendb[lax.rem(u, SEND_SLOTS), tile(q, pair), :] = dot(sel[tile(q, pair), :], z[...]).astype(BF16)
            back(u, lax.rem(2 * q - me + n, n)).start()
            back(u, lax.rem(2 * q + 1 - me + n, n)).start()

        sendb[lax.rem(u, SEND_SLOTS), tile(partner, pair_cap), :] = dot(sel[tile(partner, pair_cap), :], z[...]).astype(BF16)
        back(u, lax.rem(partner - me + n, n)).start()
        xb[u, pl.ds(pl.multiple_of(landing(me) + me * pair_cap, pair_cap), pair_cap), :] = dot(sel[tile(me, pair_cap), :], z[...]).astype(BF16)

    def weights_at(k):
        return (tok_loc if k == 1 else 0), (slots if k == 2 else 0)

    def build_weights():
        for i in range(1, n):
            meta_copy(i).wait()

        @pl.loop(0, n)
        def _(o):
            tok = 16.0 * metar[o, 0:1, :] + metar[o, 1:2, :] + metar[o, 2:3, :] - 1.0
            hit = lax.broadcasted_iota(jnp.int32, (tok_loc, pair_cap), 0).astype(F32) == tok
            for k in range(3):
                r0, c0 = weights_at(k)
                pick[pl.ds(r0, tok_loc), pl.ds(pl.multiple_of(c0 + o * pair_cap, pair_cap), pair_cap)] = jnp.where(hit, metar[o, 3 + k:4 + k, :], 0.0).astype(BF16)

    def finish(u, last=False):
        pair = 2 * pair_cap

        def shared(rows):
            return dot(hsb[rows, :], ws2[:, tile(u, UNIT)]).astype(BF16).astype(F32)

        def weighted(t, acc, q):
            for part in range(3):
                r0, c0 = weights_at(part)
                lhs_rows = pl.ds(pl.multiple_of(r0 + t * COMBINE_ROWS, COMBINE_ROWS), COMBINE_ROWS)
                if q is None:
                    acc += dot(pick[lhs_rows, c0:c0 + slots], xb[u, pl.ds(pl.multiple_of(landing(me), slots), slots), :])
                else:
                    acc += dot(pick[lhs_rows, pl.ds(pl.multiple_of(c0 + q * pair, pair), pair)], xb[u, pl.ds(pl.multiple_of(landing(me) + q * pair, pair), pair), :])
            return acc

        def write(t, acc):
            x_own = xb[u, pl.ds(pl.multiple_of(me * tok_loc + t * COMBINE_ROWS, COMBINE_ROWS), COMBINE_ROWS), :].astype(F32)
            out_ref[tile(t, COMBINE_ROWS), tile(u, UNIT)] = (x_own + acc).astype(BF16)

        def chip_arrived(q):
            arrived(u, lax.rem(me + n - 2 * q, n))
            arrived(u, lax.rem(me + n - 2 * q - 1 + n, n))

        arrived(u, lax.rem(me + n - partner, n))
        chip_arrived(near_chips[1])
        chip_arrived(near_chips[2])
        if last:
            @pl.loop(0, tok_loc // COMBINE_ROWS)
            def _(t):
                acc = shared(tile(t, COMBINE_ROWS))
                for q in near_chips:
                    acc = weighted(t, acc, q)
                hacc[tile(t, COMBINE_ROWS), 0:UNIT] = acc

            chip_arrived(far_chip)

            @pl.loop(0, tok_loc // COMBINE_ROWS)
            def _(t):
                write(t, weighted(t, hacc[tile(t, COMBINE_ROWS), 0:UNIT], far_chip))
        else:
            chip_arrived(far_chip)

            @pl.loop(0, tok_loc // COMBINE_ROWS)
            def _(t):
                write(t, weighted(t, shared(tile(t, COMBINE_ROWS)), None))


    send_back(0)
    second_product(1)
    send_back(1)
    build_weights()
    for cp in ws1_copies:
        cp.wait()
    ws2_copy.wait()

    @pl.loop(0, tok_loc // 128)
    def _(t):
        rows = pl.ds(pl.multiple_of(me * tok_loc + t * 128, 128), 128)
        acc = dot(xb[0, rows, :], w1buf[0, 0])
        for u in range(1, nu):
            acc += dot(xb[u, rows, :], w1buf[0, u])
        hsb[tile(t, 128), :] = gelu(acc).astype(BF16)


    finish(0)

    @pl.loop(2, nu)
    def _(u):
        second_product(u)
        send_back(u)
        finish(u - 1)

    finish(nu - 1, True)

    @pl.loop(nu - SEND_SLOTS, nu)
    def _(u):
        for i in range(1, n):
            back(u, i).wait_send()


def solution(mesh):
    n = mesh.shape["ep"]

    def local_layer(x_rows, logits, w_in, w_out, shared_in, shared_out):
        tok_loc, d_model = x_rows.shape
        experts = logits.shape[1]
        num_local = experts // n
        cap = tok_loc * n * CAP_FACTOR // experts
        pair_cap = 2 * tok_loc * CAP_FACTOR // n
        ff = w_in.shape[2]
        tokens, rows_total, slots = n * tok_loc, num_local * cap, n * pair_cap
        nu = d_model // UNIT
        hbm = pl.BlockSpec(memory_space=pl.ANY)
        dma = pltpu.SemaphoreType.DMA
        vmem = pltpu.VMEM
        return pl.pallas_call(
            functools.partial(layer_kernel, n),
            out_shape=pltpu.VMEM((tok_loc, d_model), BF16),
            in_specs=[hbm] * 6,
            out_specs=pl.BlockSpec(memory_space=pltpu.VMEM),
            scratch_shapes=[
                vmem((nu, tokens, UNIT), BF16),
                vmem((rows_total, tokens), BF16),
                vmem((slots, rows_total), BF16),
                vmem((SEND_SLOTS, slots, UNIT), BF16),
                vmem((2, rows_total, UNIT), BF16),
                vmem((rows_total, ff), F32),
                vmem((W1_DEPTH, EXPERT_GROUP, UNIT, ff), BF16),
                vmem((W2_DEPTH, EXPERT_GROUP, ff, UNIT), BF16),
                vmem((rows_total, UNIT), BF16),
                vmem((rows_total, ff), BF16),
                vmem((tok_loc, shared_in.shape[1]), BF16),
                vmem(shared_out.shape, BF16),
                vmem((tok_loc, experts), F32),
                vmem((tok_loc, experts), F32),
                vmem((128, experts), F32),
                vmem((n, num_local, 128), F32),
                vmem((n, num_local, 128), F32),
                vmem((n, num_local, 128), F32),
                vmem((n, num_local, 128), F32),
                vmem((n, num_local, 128), F32),
                vmem((8, rows_total), F32),
                vmem((n, 8, pair_cap), F32),
                vmem((n, 8, pair_cap), F32),
                dma((nu,)), dma((3,)), dma((n,)), dma((n,)), dma((nu, KINDS)), dma((nu, KINDS)),
                dma((W1_DEPTH,)), dma((W2_DEPTH,)), dma((n,)), dma((n,)), dma((nu, n)), dma((nu, n)), pltpu.SemaphoreType.REGULAR,
            ],
            compiler_params=pltpu.CompilerParams(collective_id=0, has_side_effects=True, vmem_limit_bytes=VMEM_BYTES),
            name="moe_layer",
        )(x_rows, logits, w_in, shared_in, w_out, shared_out)

    row_spec = P(("dp", "ep"), None)
    expert_spec = P("ep", None, None)
    return jax.shard_map(local_layer, mesh=mesh, in_specs=(row_spec, row_spec, expert_spec, expert_spec, P(None, None), P(None, None)), out_specs=row_spec, check_vma=False)
```
